512 devices in a mesh: gx: 32 (over z, x), gy: 16 (over y, core).
Axes of the slice: x: 4, y: 8, z: 8, core: 2. Of those that a mesh axis runs over, the one named last changes fastest.
Arguments:
- basis: float32 [64, 2048, 2048], P(None, 'gx', 'gy'), may hold values from -6 to 6
- panel: float32 [8, 2048, 2048], P(None, 'gx', 'gy'), may hold values from -12 to 12
- rate_codes: int32 [4, 2048, 2048], P(None, 'gx', 'gy'), may hold values from 1 to 16
Outputs:
- first_panel: float32 [8, 2048, 2048], P(None, 'gx', 'gy')
- second_panel: float32 [8, 2048, 2048], P(None, 'gx', 'gy')
- first_coef: float32 [72, 8], replicated
- second_coef: float32 [80, 8], replicated
The draws below stay inside these ranges and needn't reach their ends.
All inputs are finite; a program needn't handle non-finite values.
Results may differ from the reference program's by a relative error of at most 0.00014.
Values sent between devices are 32-bit elements; how exact they have to be, the bound alone decides.
A program may use at most 64 MiB of HBM per device.

```python
import jax
import jax.numpy as jnp
from jax import lax

BLOCK = 8
BASIS = 64
NX = 2048
NY = 2048


def basis_fields(key):
    base_key = jax.random.fold_in(key, 23)
    noise_key, shared_key, weight_key, sign_key = jax.random.split(base_key, 4)
    row_pos = jnp.arange(NX, dtype=jnp.float32) / max(NX - 1, 1)
    shared_sign = 2.0 * jax.random.bernoulli(shared_key, 0.5, (1, NX, NY)).astype(jnp.float32) - 1.0
    col_signs = 2.0 * jax.random.bernoulli(sign_key, 0.5, (BASIS, 1, 1)).astype(jnp.float32) - 1.0
    col_weights = jax.random.uniform(weight_key, (BASIS, 1, 1), jnp.float32, 0.03, 0.07) * col_signs
    noise_part = jnp.clip(jax.random.normal(noise_key, (BASIS, NX, NY), jnp.float32), -4.0, 4.0)
    amplitude = 1.0 + 3.0 * row_pos
    result = noise_part + shared_sign * col_weights * amplitude[None, :, None]
    return jnp.clip(result, -6.0, 6.0).astype(jnp.float32)


def draw_basis(key, part):
    return basis_fields(key)


def draw_panel(key, part):
    base_key = jax.random.fold_in(key, 11)
    first_key = jax.random.fold_in(base_key, 0)
    mix_key = jax.random.fold_in(base_key, 2)
    row_pos = jnp.arange(NX, dtype=jnp.float32)
    row_scale = 1.0 + 2.0 * row_pos / max(NX - 1, 1)
    values = jnp.clip(jax.random.normal(first_key, (BLOCK, NX, NY), jnp.float32), -4.0, 4.0)
    own_part = values * row_scale[None, :, None]
    mixing = jax.random.normal(mix_key, (BLOCK, BASIS), jnp.float32) * 0.15
    basis_part = jnp.einsum('jk,kxy->jxy', mixing, basis_fields(key))
    return jnp.clip(own_part + basis_part, -12.0, 12.0).astype(jnp.float32)


def touch_ends(array, rng, low, high):
    index_at = [jax.random.randint(jax.random.fold_in(rng, axis), (), 0, length) for axis, length in enumerate(array.shape)]
    widest = array.shape.index(max(array.shape))
    neighbour = index_at[:widest] + [(index_at[widest] + 1) % array.shape[widest]] + index_at[widest + 1:]
    return array.at[tuple(index_at)].set(low).at[tuple(neighbour)].set(high)


def setup_inputs(seed: int = 0) -> dict:
    seeds = jax.random.split(jax.random.key(seed), 4)
    basis = draw_basis(jax.random.fold_in(seeds[3], 71), 0)
    panel = draw_panel(jax.random.fold_in(seeds[3], 71), 0)
    rate_codes = touch_ends(jax.random.randint(seeds[2], (4, NX, NY), 1, 17), jax.random.fold_in(seeds[2], 1), 1, 16).astype(jnp.int32)
    return {"basis": basis, "panel": panel, "rate_codes": rate_codes}


HIGH = lax.Precision.HIGHEST

def lattice_apply(field, rate_codes):
    rate_vals = rate_codes.astype(jnp.float32) * 0.125
    padded = jnp.pad(field, ((0, 0), (1, 1), (1, 1)))
    rate_pad = jnp.pad(rate_vals, ((0, 0), (1, 1), (1, 1)))
    inflow = padded[:, :-2, 1:-1] * rate_pad[1, :-2, 1:-1] + padded[:, 2:, 1:-1] * rate_pad[0, 2:, 1:-1] + padded[:, 1:-1, :-2] * rate_pad[3, 1:-1, :-2] + padded[:, 1:-1, 2:] * rate_pad[2, 1:-1, 2:]
    return inflow - jnp.sum(rate_vals, axis=0) * field

def expand_once(basis_flat, panel_flat, site_count):
    proj_coef = jnp.dot(basis_flat, panel_flat.T, precision=HIGH) / site_count
    cleaned = panel_flat - jnp.dot(proj_coef.T, basis_flat, precision=HIGH)
    gram_mat = jnp.dot(cleaned, cleaned.T, precision=HIGH) / site_count
    lower_fac = jnp.linalg.cholesky(gram_mat)
    width_cols = gram_mat.shape[0]
    inverse_fac = lax.linalg.triangular_solve(lower_fac, jnp.eye(width_cols, dtype=jnp.float32), left_side=True, lower=True)
    new_panel = jnp.dot(inverse_fac, cleaned, precision=HIGH)
    return (new_panel, jnp.concatenate([proj_coef, lower_fac.T], axis=0))

def reference(basis, panel, rate_codes):
    site_count = jnp.float32(NX * NY)
    basis_flat = basis.reshape(BASIS, NX * NY)
    image_one = lattice_apply(panel, rate_codes).reshape(BLOCK, NX * NY)
    first_flat, first_coef = expand_once(basis_flat, image_one, site_count)
    first_panel = first_flat.reshape(BLOCK, NX, NY)
    image_two = lattice_apply(first_panel, rate_codes).reshape(BLOCK, NX * NY)
    grown = jnp.concatenate([basis_flat, first_flat], axis=0)
    second_flat, second_coef = expand_once(grown, image_two, site_count)
    return (first_panel, second_flat.reshape(BLOCK, NX, NY), first_coef, second_coef)
```

```python
import functools

import jax
import jax.numpy as jnp
from jax import lax
from jax.experimental import pallas as pl
from jax.experimental.pallas import tpu as pltpu
from jax.sharding import PartitionSpec as P

HIGH = lax.Precision.HIGHEST
MESH = pl.DeviceIdType.MESH
F32 = jnp.float32
BF16 = jnp.bfloat16
NN = (((1,), (0,)), ((), ()))
NT = (((1,), (1,)), ((), ()))
LANES = 128


def small_dot(a, b, dims):
    return lax.dot_general(a, b, dims, precision=HIGH, preferred_element_type=F32)


def split_two(x):
    hi = x.astype(BF16)
    lo = (x - hi.astype(F32)).astype(BF16)
    return hi, lo


def eliminate(gram):
    n = gram.shape[0]
    row = lax.broadcasted_iota(jnp.int32, (n, n), 0)
    col = lax.broadcasted_iota(jnp.int32, (n, n), 1)
    left = gram
    right = jnp.where(row == col, 1.0, 0.0).astype(F32)
    for j in range(n):
        factor = jnp.where(row[:, :1] > j, left[:, j : j + 1] / left[j : j + 1, j : j + 1], 0.0)
        left, right = (left - factor * left[j : j + 1, :], right - factor * right[j : j + 1, :])
    diag = jnp.sum(jnp.where(row == col, left, 0.0), axis=1, keepdims=True)
    root = 1.0 / jnp.sqrt(diag)
    return jnp.where(row <= col, left * root, 0.0), right * root


def kernel(
    dims,
    xb_ref, xp_ref, codes_ref,
    q1_ref, q2_ref, co_ref, lt_ref,
    rf, up_x, dn_x, up_r, dn_r, pack_l, pack_r, from_l, from_r,
    w1, up_w, dn_w, wpack_l, wpack_r, wfrom_l, wfrom_r,
    z2, acc, payload, rs_buf, y_buf, z_buf, full,
    halo_send, halo_recv, red_send, red_recv,
):
    nz, nx, ny, rows, nb, np_, scale = dims
    nm = nx * 2
    chunk = payload.shape[0] // nm
    gx, gy = lax.axis_index("gx"), lax.axis_index("gy")
    zz, xx = gx // nx, gx % nx
    yy, core = gy // 2, gy % 2
    member = xx * 2 + core
    ngx, ngy = nz * nx, ny * 2
    above = ((gx + ngx - 1) % ngx, gy)
    below = ((gx + 1) % ngx, gy)
    left = (gx, (gy + ngy - 1) % ngy)
    right = (gx, (gy + 1) % ngy)

    def in_team(d):
        m = (member + d) % nm
        return (zz * nx + m // 2, yy * 2 + m % 2)

    def in_y(d):
        return (gx, ((yy + d) % ny) * 2 + core)

    def in_z(d):
        return (((zz + d) % nz) * nx + xx, gy)

    peers = [above, below, left, right]
    peers += [in_team(d) for d in range(1, nm)]
    peers += [in_y(d) for d in range(1, ny)]
    peers += [in_z(d) for d in range(1, nz)]
    barrier = pltpu.get_barrier_semaphore()
    for peer in peers:
        pl.semaphore_signal(barrier, inc=1, device_id=peer, device_id_type=MESH)

    nc = nb + np_
    nt = nb * 2 + np_ * 2
    lane = lax.broadcasted_iota(jnp.int32, (1, LANES), 1)

    codes = codes_ref[...].astype(F32) * 0.125
    rf[0:4] = codes
    rf[4] = codes[0] + codes[1] + codes[2] + codes[3]

    def rate(d, r):
        return rf[d, pl.ds(r, 1), :]

    def cols(ref, r):
        return ref[:, pl.ds(pl.multiple_of(r * LANES, LANES), LANES)]

    def pack_step(x, r, accs):
        y = jnp.where(lane == LANES - 1, rate(3, r) * x, rate(2, r) * x)
        y = pltpu.roll(y, r, 1)
        a, b = accs
        return (jnp.where(lane == r, y, a), jnp.where(lane == (r + LANES - 1) % LANES, y, b))

    def pack_b(r, accs):
        return pack_step(cols(xb_ref, r), r, accs)

    def pack_p(r, accs):
        return pack_step(cols(xp_ref, r), r, accs)

    zp = jnp.zeros((np_, LANES), F32)
    zb = jnp.zeros((nb, LANES), F32)
    a, b = lax.fori_loop(0, rows, pack_p, (zp, zp))
    pack_l[nb:nc] = a
    pack_r[nb:nc] = b
    a, b = lax.fori_loop(0, rows, pack_b, (zb, zb))
    pack_l[0:nb] = a
    pack_r[0:nb] = b

    pl.semaphore_wait(barrier, len(peers))

    last = (rows - 1) * LANES
    end = rows * LANES

    def halo(k, src, dst, peer):
        c = pltpu.make_async_remote_copy(
            src_ref=src, dst_ref=dst, send_sem=halo_send.at[k], recv_sem=halo_recv.at[k],
            device_id=peer, device_id_type=MESH,
        )
        c.start()
        return c

    small = [
        halo(0, xp_ref.at[:, last:end], up_x.at[nb:nc], below),
        halo(1, xp_ref.at[:, 0:LANES], dn_x.at[nb:nc], above),
        halo(2, pack_r.at[nb:nc], from_l.at[nb:nc], right),
        halo(3, pack_l.at[nb:nc], from_r.at[nb:nc], left),
        halo(4, codes_ref.at[1, rows - 8 : rows], up_r, below),
        halo(5, codes_ref.at[0, 0:8], dn_r, above),
    ]
    big = [
        halo(6, xb_ref.at[:, last:end], up_x.at[0:nb], below),
        halo(7, xb_ref.at[:, 0:LANES], dn_x.at[0:nb], above),
        halo(8, pack_r.at[0:nb], from_l.at[0:nb], right),
        halo(9, pack_l.at[0:nb], from_r.at[0:nb], left),
    ]

    def put(first, r, x):
        hi, lo = split_two(x)
        at = pl.ds(pl.multiple_of(r * LANES, LANES), LANES)
        z2[first : first + x.shape[0], at] = hi
        z2[nt + first : nt + first + x.shape[0], at] = lo

    def split_b(r, _):
        put(0, r, cols(xb_ref, r))
        return 0

    lax.fori_loop(0, rows, split_b, 0)

    def stencil(r, rate_u, rate_d, xu, x, xd, fl, fr):
        from_l = jnp.where(lane == 0, pltpu.roll(fl, (2 * LANES + 1 - r) % LANES, 1), pltpu.roll(rate(3, r) * x, 1, 1))
        from_r = jnp.where(
            lane == LANES - 1, pltpu.roll(fr, (2 * LANES - 1 - r) % LANES, 1), pltpu.roll(rate(2, r) * x, LANES - 1, 1)
        )
        return (rate_u * xu + rate_d * xd) + (from_l + from_r) - rate(4, r) * x

    def sweep(x_at, up, dn, fl, fr, emit, carry, unroll):
        e = rows - 1

        def group(rs, c):
            outs = []
            for r in rs:
                at_top, at_end = isinstance(r, int) and r == 0, isinstance(r, int) and r == e
                outs.append(
                    stencil(
                        r,
                        rate_up() if at_top else rate(1, r - 1),
                        rate_dn() if at_end else rate(0, r + 1),
                        up if at_top else x_at(r - 1),
                        x_at(r),
                        dn if at_end else x_at(r + 1),
                        fl, fr,
                    )
                )
            for r, out in zip(rs, outs):
                c = emit(r, out, c)
            return c

        trips = (rows - 2) // unroll
        carry = lax.fori_loop(
            0, trips, lambda k, c: group([1 + k * unroll + i for i in range(unroll)], c), carry
        )
        return group([0] + list(range(1 + trips * unroll, rows)), carry)

    def rate_up():
        return up_r[7:8, :].astype(F32) * 0.125

    def rate_dn():
        return dn_r[0:1, :].astype(F32) * 0.125

    keep = (gx > 0, gx < ngx - 1, gy > 0, gy < ngy - 1)

    def edged(values):
        return [v * jnp.where(k, 1.0, 0.0).astype(F32) for v, k in zip(values, keep)]

    for c in small:
        c.wait()

    def emit_w(r, out, accs):
        w1[:, pl.ds(pl.multiple_of(r * LANES, LANES), LANES)] = out
        return pack_step(out, r, accs)

    halos = edged([up_x[nb:nc], dn_x[nb:nc], from_l[nb:nc], from_r[nb:nc]])
    a, b = sweep(lambda r: cols(xp_ref, r), *halos, emit_w, (zp, zp), 12)
    wpack_l[...] = a
    wpack_r[...] = b
    wsend = [
        halo(10, w1.at[:, last:end], up_w, below),
        halo(11, w1.at[:, 0:LANES], dn_w, above),
        halo(12, wpack_r, wfrom_l, right),
        halo(13, wpack_l, wfrom_r, left),
    ]

    for c in big:
        c.wait()

    def emit_b(r, out, c):
        put(nb, r, out)
        return c

    halos = edged([up_x[0:nb], dn_x[0:nb], from_l[0:nb], from_r[0:nb]])
    sweep(lambda r: cols(xb_ref, r), *halos, emit_b, 0, 2)

    for c in wsend:
        c.wait()

    def emit_aw(r, out, c):
        put(2 * nb, r, jnp.concatenate([cols(w1, r), out], axis=0))
        return c

    halos = edged([up_w[...], dn_w[...], wfrom_l[...], wfrom_r[...]])
    sweep(lambda r: cols(w1, r), *halos, emit_aw, 0, 12)

    step = min(1024, end)
    acc[...] = jnp.zeros_like(acc)

    def gram_step(k, _):
        at = pl.ds(pl.multiple_of(k * step, step), step)
        acc[...] += lax.dot_general(z2[:, at], z2[0:nt, at], NT, preferred_element_type=F32)
        return 0

    lax.fori_loop(0, end // step, gram_step, 0)
    half = acc[0:nt, :] * 0.5 + acc[nt : 2 * nt, :]
    na = 2 * nb
    aa = half[0:na, 0:na]
    aa = aa + aa.T
    aw = jnp.concatenate([half[0:na, na:nt], jnp.zeros((na, LANES - (nt - na)), F32)], axis=1)
    wa = half[na:nt, 0:na] + aw.T[0 : nt - na, :]
    ww = half[na:nt, na:nt]
    ww = ww + ww.T
    lane_low = lane < nb
    payload[0:nb] = aa[0:nb]
    hb = nb // 2
    payload[nb : nb + hb] = jnp.where(lane_low, pltpu.roll(aa[nb : nb + hb], nb, 1), aa[nb + hb : na])
    base = nb + hb
    payload[base : base + 2 * np_] = wa
    payload[base + 2 * np_ : base + 4 * np_] = jnp.concatenate(
        [ww, jnp.zeros((2 * np_, LANES - 2 * np_), F32)], axis=1
    )

    def reduce_copy(k, src, dst, peer):
        c = pltpu.make_async_remote_copy(
            src_ref=src, dst_ref=dst, send_sem=red_send.at[k], recv_sem=red_recv.at[k],
            device_id=peer, device_id_type=MESH,
        )
        c.start()
        return c

    def piece(m):
        return pl.ds(pl.multiple_of(m * chunk, chunk), chunk)

    copies = []
    for d in range(1, nm):
        copies.append(reduce_copy(d, payload.at[piece((member + d) % nm)], rs_buf.at[member], in_team(d)))
    rs_buf[member] = payload[piece(member)]
    for c in copies:
        c.wait()

    def ordered_sum(buf, n):
        total = buf[0]
        for i in range(1, n):
            total = total + buf[i]
        return total

    y_buf[yy] = ordered_sum(rs_buf, nm)
    copies = [reduce_copy(nm + d, y_buf.at[yy], y_buf.at[yy], in_y(d)) for d in range(1, ny)]
    for c in copies:
        c.wait()
    z_buf[zz] = ordered_sum(y_buf, ny)
    copies = [reduce_copy(nm + ny + d, z_buf.at[zz], z_buf.at[zz], in_z(d)) for d in range(1, nz)]
    for c in copies:
        c.wait()
    full[piece(member)] = ordered_sum(z_buf, nz)
    copies = [
        reduce_copy(nm + ny + nz + d, full.at[piece(member)], full.at[piece(member)], in_team(d))
        for d in range(1, nm)
    ]
    for c in copies:
        c.wait()

    g = full[...] * scale
    gb = g[0:nb]
    ap = g[nb : nb + hb]
    ga_rows = jnp.concatenate([gb, pltpu.roll(ap, nb, 1), ap], axis=0)
    wa = g[base : base + 2 * np_]
    ww = g[base + 2 * np_ : base + 4 * np_]
    w1a, w2a = wa[0:np_], wa[np_:]
    n2 = 2 * np_
    h1 = jnp.where(lane_low, w1a, 0.0)
    v_a = w1a - small_dot(h1[:, 0:nb], gb, NN)
    v_w = ww[0:np_, 0:n2] - small_dot(h1, wa, NT)
    gram = v_w[:, 0:np_] - small_dot(v_a, h1, NT)
    lt1, li1 = eliminate(gram)
    t_b = -small_dot(li1, h1, NN)
    t_a = small_dot(li1, v_a, NN)
    t_w = small_dot(li1, v_w, NN)
    u_a = pltpu.roll(t_b, nb, 1)
    gu_a = small_dot(u_a, ga_rows, NT) + small_dot(li1, w2a, NN)
    gu_w = small_dot(u_a, wa, NT) + small_dot(li1, ww[np_:, 0:n2], NN)
    h2b = jnp.where(lane_low, gu_a, 0.0)
    h2q = small_dot(h2b, t_b, NT) + small_dot(gu_w[:, 0:np_], li1, NT)
    c2a = u_a - h2b - small_dot(h2q, t_b, NN)
    c2w = -small_dot(h2q, li1, NN)
    g2a = gu_a - small_dot(h2b[:, 0:nb], gb, NN) - small_dot(h2q, t_a, NN)
    g2w = gu_w - small_dot(h2b, wa, NT) - small_dot(h2q, t_w, NN)
    gram = small_dot(c2a, g2a, NT) + small_dot(c2w, g2w[:, 0:np_], NT) + small_dot(li1, g2w[:, np_:], NT)
    lt2, li2 = eliminate(gram)
    d_a = small_dot(li2, c2a, NN)
    d_w = small_dot(li2, c2w, NN)
    d_v = small_dot(li2, li1, NN)
    zero = jnp.zeros((np_, np_), F32)
    coef_a = jnp.concatenate([t_b, d_a], axis=0)
    coef_w = jnp.concatenate(
        [jnp.concatenate([li1, zero], axis=1), jnp.concatenate([d_w, d_v], axis=1)], axis=0
    )
    coef = jnp.concatenate([coef_a, coef_w], axis=1)
    c_hi, c_mid = split_two(coef)
    c_lo = (coef - c_hi.astype(F32) - c_mid.astype(F32)).astype(BF16)
    three = jnp.concatenate([c_hi, c_mid, c_lo], axis=0)
    two = jnp.concatenate([c_hi, c_mid], axis=0)
    width = min(512, end)

    def last_step(k, _):
        at = pl.ds(pl.multiple_of(k * width, width), width)
        o = lax.dot_general(three, z2[0:nt, at], NN, preferred_element_type=F32)
        p = lax.dot_general(two, z2[nt : 2 * nt, at], NN, preferred_element_type=F32)
        out = o[0:n2] + ((o[n2 : 2 * n2] + p[0:n2]) + (o[2 * n2 :] + p[n2:]))
        q1_ref[:, at] = out[0:np_]
        q2_ref[:, at] = out[np_:]
        return 0

    lax.fori_loop(0, end // width, last_step, 0)
    co_ref[0:np_] = h1
    co_ref[np_:n2] = h2b
    pad = jnp.zeros((np_, LANES - np_), F32)
    lt_ref[0:np_] = jnp.concatenate([lt1, pad], axis=1)
    lt_ref[np_:n2] = jnp.concatenate([lt2, pad], axis=1)
    lt_ref[n2 : n2 + np_] = jnp.concatenate([h2q, pad], axis=1)


def local(nz, nx, ny, basis, panel, rate_codes):
    nb, rows, width = basis.shape
    np_ = panel.shape[0]
    sites = rows * width * nz * nx * ny * 2
    nc, nt, flat, nm = nb + np_, 2 * nb + 2 * np_, rows * width, nx * 2
    dims = (nz, nx, ny, rows, nb, np_, 1.0 / sites)
    vm = pltpu.VMEM
    tile = lambda n: vm((n, LANES), F32)
    scratch = [
        vm((5, rows, LANES), F32),
        tile(nc), tile(nc), vm((8, LANES), jnp.int32), vm((8, LANES), jnp.int32),
        tile(nc), tile(nc), tile(nc), tile(nc),
        vm((np_, flat), F32), tile(np_), tile(np_), tile(np_), tile(np_), tile(np_), tile(np_),
        vm((2 * nt, flat), BF16), vm((2 * nt, nt), F32),
        tile(128), vm((nm, 128 // nm, LANES), F32), vm((ny, 128 // nm, LANES), F32),
        vm((nz, 128 // nm, LANES), F32), tile(128),
        pltpu.SemaphoreType.DMA((14,)), pltpu.SemaphoreType.DMA((14,)),
        pltpu.SemaphoreType.DMA((2 * nm + ny + nz,)), pltpu.SemaphoreType.DMA((2 * nm + ny + nz,)),
    ]
    spec = pl.BlockSpec(memory_space=pltpu.VMEM)
    q1, q2, co, lt = pl.pallas_call(
        functools.partial(kernel, dims),
        out_shape=(
            jax.ShapeDtypeStruct((np_, flat), F32),
            jax.ShapeDtypeStruct((np_, flat), F32),
            jax.ShapeDtypeStruct((2 * np_, LANES), F32),
            jax.ShapeDtypeStruct((3 * np_, LANES), F32),
        ),
        in_specs=[spec] * 3,
        out_specs=(spec,) * 4,
        scratch_shapes=scratch,
        compiler_params=pltpu.CompilerParams(collective_id=0, has_side_effects=True, vmem_limit_bytes=32 << 20),
        cost_estimate=pl.CostEstimate(flops=10**9, bytes_accessed=4 << 20, transcendentals=0),
    )(basis.reshape(nb, flat), panel.reshape(np_, flat), rate_codes)
    first = jnp.concatenate([co[0:np_, 0:nb].T, lt[0:np_, 0:np_]], axis=0)
    second = jnp.concatenate(
        [co[np_:, 0:nb].T, lt[2 * np_ :, 0:np_].T, lt[np_ : 2 * np_, 0:np_]], axis=0
    )
    return (q1.reshape(np_, rows, width), q2.reshape(np_, rows, width), first, second)


def solution(mesh):
    nx = 4
    nz = mesh.shape["gx"] // nx
    ny = mesh.shape["gy"] // 2
    placed = P(None, "gx", "gy")
    return jax.shard_map(
        functools.partial(local, nz, nx, ny),
        mesh=mesh,
        in_specs=(placed, placed, placed),
        out_specs=(placed, placed, P(), P()),
        check_vma=False,
    )
```

```python
import functools

import jax
import jax.numpy as jnp
from jax import lax
from jax.experimental import pallas as pl
from jax.experimental.pallas import tpu as pltpu
from jax.sharding import PartitionSpec as P

HIGH = lax.Precision.HIGHEST
MESH = pl.DeviceIdType.MESH
F32 = jnp.float32
BF16 = jnp.bfloat16
NN = (((1,), (0,)), ((), ()))
NT = (((1,), (1,)), ((), ()))
LANES = 128


def small_dot(a, b, dims):
    return lax.dot_general(a, b, dims, precision=HIGH, preferred_element_type=F32)


def split_two(x):
    hi = x.astype(BF16)
    lo = (x - hi.astype(F32)).astype(BF16)
    return hi, lo


def eliminate(gram):
    n = gram.shape[0]
    row = lax.broadcasted_iota(jnp.int32, (n, n), 0)
    col = lax.broadcasted_iota(jnp.int32, (n, n), 1)
    left = gram
    right = jnp.where(row == col, 1.0, 0.0).astype(F32)
    for j in range(n):
        factor = jnp.where(row[:, :1] > j, left[:, j : j + 1] / left[j : j + 1, j : j + 1], 0.0)
        left, right = (left - factor * left[j : j + 1, :], right - factor * right[j : j + 1, :])
    diag = jnp.sum(jnp.where(row == col, left, 0.0), axis=1, keepdims=True)
    root = 1.0 / jnp.sqrt(diag)
    return jnp.where(row <= col, left * root, 0.0), right * root


def kernel(
    dims,
    b_hbm, p_hbm, codes_hbm,
    q1_ref, q2_ref, c1_ref, c2_ref,
    xt, wt, codes, rf, up_r, dn_r, pack_l, pack_r, from_l, from_r, wpack_l, wpack_r, wfrom_l, wfrom_r,
    z2, acc, payload, rs_buf, a_buf, b_buf, full,
    load_sem, halo_send, halo_recv, red_send, red_recv,
):
    nz, nx, ny, rows, nb, np_, scale = dims
    nm = nx * 2
    gx, gy = lax.axis_index("gx"), lax.axis_index("gy")
    zz, xx = gx // nx, gx % nx
    yy, core = gy // 2, gy % 2
    member = xx * 2 + core
    ngx, ngy = nz * nx, ny * 2
    above = ((gx + ngx - 1) % ngx, gy)
    below = ((gx + 1) % ngx, gy)
    left = (gx, (gy + ngy - 1) % ngy)
    right = (gx, (gy + 1) % ngy)

    def in_team(d):
        m = (member + d) % nm
        return (zz * nx + m // 2, yy * 2 + m % 2)

    def in_y(d):
        return (gx, ((yy + d) % ny) * 2 + core)

    def in_z(d):
        return (((zz + d) % nz) * nx + xx, gy)

    def in_first(d):
        a, b = in_y(d), in_z(d)
        return (a[0] * (1 - core) + b[0] * core, a[1] * (1 - core) + b[1] * core)

    def in_second(d):
        a, b = in_z(d), in_y(d)
        return (a[0] * (1 - core) + b[0] * core, a[1] * (1 - core) + b[1] * core)

    peers = [above, below, left, right]
    peers += [in_team(d) for d in range(1, nm)]
    peers += [in_y(d) for d in range(1, ny)]
    peers += [in_z(d) for d in range(1, nz)]
    barrier = pltpu.get_barrier_semaphore()
    for peer in peers:
        pl.semaphore_signal(barrier, inc=1, device_id=peer, device_id_type=MESH)

    nc = nb + np_
    nt = nb * 2 + np_ * 2
    inner = slice(1, rows + 1)
    load_codes = pltpu.make_async_copy(codes_hbm, codes, load_sem.at[0])
    load_codes.start()
    for c in range(np_):
        pltpu.make_async_copy(p_hbm.at[c], xt.at[inner, nb + c], load_sem.at[1]).start()
    for c in range(nb):
        pltpu.make_async_copy(b_hbm.at[c], xt.at[inner, c], load_sem.at[2]).start()

    lane = lax.broadcasted_iota(jnp.int32, (1, LANES), 1)
    top = 8

    def rate(d, r):
        return rf[d, pl.ds(r + top, 1), :]

    def pack_step(x, r, accs):
        y = jnp.where(lane == LANES - 1, rate(3, r) * x, rate(2, r) * x)
        y = pltpu.roll(y, r, 1)
        a, b = accs
        return (jnp.where(lane == r, y, a), jnp.where(lane == (r + LANES - 1) % LANES, y, b))

    def pack(at, n):
        per = 8

        def body(k, accs):
            for i in range(per):
                accs = pack_step(xt[k * per + i + 1, at], k * per + i, accs)
            return accs

        zero = jnp.zeros((n, LANES), F32)
        a, b = lax.fori_loop(0, rows // per, body, (zero, zero))
        pack_l[at] = a
        pack_r[at] = b

    load_codes.wait()
    values = codes[...].astype(F32) * 0.125
    rf[0:4, top : top + rows] = values
    rf[4, top : top + rows] = values[0] + values[1] + values[2] + values[3]
    pltpu.make_async_copy(p_hbm, xt.at[inner, nb:nc], load_sem.at[1]).wait()
    pack(slice(nb, nc), np_)

    pl.semaphore_wait(barrier, len(peers))

    def halo(k, src, dst, peer):
        c = pltpu.make_async_remote_copy(
            src_ref=src, dst_ref=dst, send_sem=halo_send.at[k], recv_sem=halo_recv.at[k],
            device_id=peer, device_id_type=MESH,
        )
        c.start()
        return c

    small = [
        halo(0, xt.at[rows, nb:nc], xt.at[0, nb:nc], below),
        halo(1, xt.at[1, nb:nc], xt.at[rows + 1, nb:nc], above),
        halo(2, pack_r.at[nb:nc], from_l.at[nb:nc], right),
        halo(3, pack_l.at[nb:nc], from_r.at[nb:nc], left),
        halo(4, codes.at[1, rows - 8 : rows], up_r, below),
        halo(5, codes.at[0, 0:8], dn_r, above),
    ]
    pltpu.make_async_copy(b_hbm, xt.at[inner, 0:nb], load_sem.at[2]).wait()
    big = [
        halo(6, xt.at[rows, 0:nb], xt.at[0, 0:nb], below),
        halo(7, xt.at[1, 0:nb], xt.at[rows + 1, 0:nb], above),
    ]
    pack(slice(0, nb), nb)
    big += [
        halo(8, pack_r.at[0:nb], from_l.at[0:nb], right),
        halo(9, pack_l.at[0:nb], from_r.at[0:nb], left),
    ]

    def put(first, r, x):
        hi, lo = split_two(x)
        at = pl.ds(pl.multiple_of(r * LANES, LANES), LANES)
        z2[first : first + x.shape[0], at] = hi
        z2[nt + first : nt + first + x.shape[0], at] = lo

    def split_b(k, _):
        for i in range(2):
            put(0, 2 * k + i, xt[2 * k + i + 1, 0:nb])
        return 0

    lax.fori_loop(0, rows // 2, split_b, 0)

    def stencil(r, xu, x, xd, fl, fr):
        from_l = jnp.where(lane == 0, pltpu.roll(fl, (2 * LANES + 1 - r) % LANES, 1), pltpu.roll(rate(3, r) * x, 1, 1))
        from_r = jnp.where(
            lane == LANES - 1, pltpu.roll(fr, (2 * LANES - 1 - r) % LANES, 1), pltpu.roll(rate(2, r) * x, LANES - 1, 1)
        )
        return (rate(1, r - 1) * xu + rate(0, r + 1) * xd) + (from_l + from_r) - rate(4, r) * x

    def sweep(x_at, fl, fr, emit, carry, per):
        def body(k, c):
            rs = [k * per + i for i in range(per)]
            outs = [stencil(r, x_at(r - 1), x_at(r), x_at(r + 1), fl, fr) for r in rs]
            for r, out in zip(rs, outs):
                c = emit(r, out, c)
            return c

        return lax.fori_loop(0, rows // per, body, carry)

    def present(k):
        return jnp.where(k, 1.0, 0.0).astype(F32)

    has_l, has_r = present(gy > 0), present(gy < ngy - 1)
    for c in small:
        c.wait()
    rf[1, top - 1 : top] = up_r[7:8].astype(F32) * 0.125 * present(gx > 0)
    rf[0, top + rows : top + rows + 1] = dn_r[0:1].astype(F32) * 0.125 * present(gx < ngx - 1)

    def emit_w(r, out, accs):
        wt[r + 1] = out
        return pack_step(out, r, accs)

    zp = jnp.zeros((np_, LANES), F32)
    a, b = sweep(lambda r: xt[r + 1, nb:nc], from_l[nb:nc] * has_l, from_r[nb:nc] * has_r, emit_w, (zp, zp), 16)
    wpack_l[...] = a
    wpack_r[...] = b
    wsend = [
        halo(10, wt.at[rows], wt.at[0], below),
        halo(11, wt.at[1], wt.at[rows + 1], above),
        halo(12, wpack_r, wfrom_l, right),
        halo(13, wpack_l, wfrom_r, left),
    ]

    for c in big:
        c.wait()

    def emit_b(r, out, c):
        put(nb, r, out)
        return c

    sweep(lambda r: xt[r + 1, 0:nb], from_l[0:nb] * has_l, from_r[0:nb] * has_r, emit_b, 0, 2)

    for c in wsend:
        c.wait()

    def emit_aw(r, out, c):
        put(2 * nb, r, jnp.concatenate([wt[r + 1], out], axis=0))
        return c

    sweep(lambda r: wt[r + 1], wfrom_l[...] * has_l, wfrom_r[...] * has_r, emit_aw, 0, 16)

    end = rows * LANES
    step = min(1024, end)
    acc[...] = jnp.zeros_like(acc)

    def gram_step(k, _):
        at = pl.ds(pl.multiple_of(k * step, step), step)
        acc[...] += lax.dot_general(z2[:, at], z2[0:nt, at], NT, preferred_element_type=F32)
        return 0

    lax.fori_loop(0, end // step, gram_step, 0)
    na, n2 = 2 * nb, 2 * np_
    half = acc[0:nt, :] * 0.5 + acc[nt : 2 * nt, :]
    aa = half[0:na, 0:na]
    aa = aa + aa.T
    aw = jnp.concatenate([half[0:na, na:nt], jnp.zeros((na, LANES - n2), F32)], axis=1)
    wa = half[na:nt, 0:na] + aw.T[0:n2, :]
    ww = half[na:nt, na:nt]
    ww = ww + ww.T
    low = lane < nb
    site = lax.broadcasted_iota(jnp.int32, (nb, LANES), 0)
    upper, same = lane >= site, lane == site
    ab_ab = pltpu.roll(aa[nb:na], nb, 1)
    main = jnp.where(low & ~upper, ab_ab, aa[0:nb])
    diag = jnp.sum(jnp.where(same, ab_ab, 0.0), axis=0, keepdims=True)
    extra = jnp.concatenate(
        [
            wa,
            jnp.concatenate([ww[0:np_], ww[np_:n2], jnp.zeros((np_, LANES - 2 * n2), F32)], axis=1),
            jnp.broadcast_to(diag, (8, LANES)),
        ],
        axis=0,
    )
    per_main, per_extra = nb // nm, 32 // nm
    per_all = per_main + per_extra
    for m in range(nm):
        payload[m, 0:per_main] = main[m * per_main : (m + 1) * per_main]
        payload[m, per_main:per_all] = extra[m * per_extra : (m + 1) * per_extra]

    def reduce_copy(k, src, dst, peer):
        c = pltpu.make_async_remote_copy(
            src_ref=src.at[0:per_all], dst_ref=dst.at[0:per_all], send_sem=red_send.at[k], recv_sem=red_recv.at[k],
            device_id=peer, device_id_type=MESH,
        )
        c.start()
        return c

    copies = []
    for d in range(1, nm):
        copies.append(reduce_copy(d, payload.at[(member + d) % nm], rs_buf.at[member], in_team(d)))
    rs_buf[member, 0:per_all] = payload[member, 0:per_all]
    for c in copies:
        c.wait()

    def ordered_sum(buf, n):
        total = buf[0, 0:per_all]
        for i in range(1, n):
            total = total + buf[i, 0:per_all]
        return total

    one = yy * (1 - core) + zz * core
    two = zz * (1 - core) + yy * core
    a_buf[one, 0:per_all] = ordered_sum(rs_buf, nm)
    copies = [reduce_copy(nm + d, a_buf.at[one], a_buf.at[one], in_first(d)) for d in range(1, ny)]
    for c in copies:
        c.wait()
    b_buf[two, 0:per_all] = ordered_sum(a_buf, ny)
    copies = [reduce_copy(nm + ny + d, b_buf.at[two], b_buf.at[two], in_second(d)) for d in range(1, nz)]
    for c in copies:
        c.wait()
    full[member, 0:per_all] = ordered_sum(b_buf, nz)
    copies = [
        reduce_copy(nm + ny + nz + d, full.at[member], full.at[member], in_team(d)) for d in range(1, nm)
    ]
    for c in copies:
        c.wait()

    main = jnp.concatenate([full[m, 0:per_main] for m in range(nm)], axis=0) * scale
    extra = jnp.concatenate([full[m, per_main:per_all] for m in range(nm)], axis=0) * scale
    wa = extra[0:n2]
    ww = extra[n2 : n2 + np_]
    diag = extra[n2 + np_ : n2 + np_ + 1]
    square = jnp.where(low, main, 0.0)
    flip = jnp.concatenate([square, jnp.zeros_like(square)], axis=0).T[0:nb]
    gb = jnp.where(low & ~upper, flip, main)
    ab_ab = jnp.where(low, jnp.where(upper, jnp.where(same, diag, flip), square), 0.0)
    ga_rows = jnp.concatenate([gb, pltpu.roll(ab_ab, nb, 1)], axis=0)
    w1a, w2a = wa[0:np_], wa[np_:]
    h1 = jnp.where(low, w1a, 0.0)
    v_a = w1a - small_dot(h1[:, 0:nb], gb, NN)
    v_w = ww[:, 0:n2] - small_dot(h1, wa, NT)
    gram = v_w[:, 0:np_] - small_dot(v_a, h1, NT)
    lt1, li1 = eliminate(gram)
    t_b = -small_dot(li1, h1, NN)
    t_a = small_dot(li1, v_a, NN)
    t_w = small_dot(li1, v_w, NN)
    u_a = pltpu.roll(t_b, nb, 1)
    gu_a = small_dot(u_a, ga_rows, NT) + small_dot(li1, w2a, NN)
    gu_w = small_dot(u_a, wa, NT) + small_dot(li1, ww[:, n2 : 2 * n2], NN)
    h2b = jnp.where(low, gu_a, 0.0)
    h2q = small_dot(h2b, t_b, NT) + small_dot(gu_w[:, 0:np_], li1, NT)
    c2a = u_a - h2b - small_dot(h2q, t_b, NN)
    c2w = -small_dot(h2q, li1, NN)
    g2a = gu_a - small_dot(h2b[:, 0:nb], gb, NN) - small_dot(h2q, t_a, NN)
    g2w = gu_w - small_dot(h2b, wa, NT) - small_dot(h2q, t_w, NN)
    gram = small_dot(c2a, g2a, NT) + small_dot(c2w, g2w[:, 0:np_], NT) + small_dot(li1, g2w[:, np_:], NT)
    lt2, li2 = eliminate(gram)
    d_a = small_dot(li2, c2a, NN)
    d_w = small_dot(li2, c2w, NN)
    d_v = small_dot(li2, li1, NN)
    zero = jnp.zeros((np_, np_), F32)
    coef_a = jnp.concatenate([t_b, d_a], axis=0)
    coef_w = jnp.concatenate(
        [jnp.concatenate([li1, zero], axis=1), jnp.concatenate([d_w, d_v], axis=1)], axis=0
    )
    coef = jnp.concatenate([coef_a, coef_w], axis=1)
    c_hi, c_mid = split_two(coef)
    c_lo = (coef - c_hi.astype(F32) - c_mid.astype(F32)).astype(BF16)
    three = jnp.concatenate([c_hi, c_mid, c_lo], axis=0)
    pair = jnp.concatenate([c_hi, c_mid], axis=0)
    per = min(4, rows)
    width = per * LANES

    def last_step(k, _):
        at = pl.ds(pl.multiple_of(k * width, width), width)
        o = lax.dot_general(three, z2[0:nt, at], NN, preferred_element_type=F32)
        p = lax.dot_general(pair, z2[nt : 2 * nt, at], NN, preferred_element_type=F32)
        out = o[0:n2] + ((o[n2 : 2 * n2] + p[0:n2]) + (o[2 * n2 :] + p[n2:]))
        for i in range(per):
            q1_ref[:, k * per + i, :] = out[0:np_, i * LANES : (i + 1) * LANES]
            q2_ref[:, k * per + i, :] = out[np_:, i * LANES : (i + 1) * LANES]
        return 0

    lax.fori_loop(0, rows // per, last_step, 0)

    def placed(x, first):
        wide = jnp.concatenate([x, jnp.zeros((np_, LANES - np_), F32)], axis=1)
        return pltpu.roll(wide, first, 1)

    c1_ref[...] = (h1 + placed(lt1.T, nb))[:, 0:nc]
    c2_ref[...] = (h2b + placed(h2q, nb) + placed(lt2.T, nc))[:, 0 : nc + np_]


def local(nz, nx, ny, basis, panel, rate_codes):
    nb, rows, width = basis.shape
    np_ = panel.shape[0]
    sites = rows * width * nz * nx * ny * 2
    nc, nt, flat, nm = nb + np_, 2 * nb + 2 * np_, rows * width, nx * 2
    dims = (nz, nx, ny, rows, nb, np_, 1.0 / sites)
    vm = pltpu.VMEM
    tile = lambda *n: vm((*n, LANES), F32)
    dma = pltpu.SemaphoreType.DMA
    scratch = [
        tile(rows + 2, nc), tile(rows + 2, np_), vm((4, rows, LANES), jnp.int32), tile(5, rows + 16),
        vm((8, LANES), jnp.int32), vm((8, LANES), jnp.int32),
        tile(nc), tile(nc), tile(nc), tile(nc), tile(np_), tile(np_), tile(np_), tile(np_),
        vm((2 * nt, flat), BF16), vm((2 * nt, nt), F32),
        tile(nm, 16), tile(nm, 16), tile(ny, 16), tile(nz, 16), tile(nm, 16),
        dma((3,)), dma((14,)), dma((14,)), dma((2 * nm + ny + nz,)), dma((2 * nm + ny + nz,)),
    ]
    vmem = pl.BlockSpec(memory_space=pltpu.VMEM)
    q1, q2, c1, c2 = pl.pallas_call(
        functools.partial(kernel, dims),
        out_shape=(
            jax.ShapeDtypeStruct((np_, rows, width), F32),
            jax.ShapeDtypeStruct((np_, rows, width), F32),
            jax.ShapeDtypeStruct((np_, nc), F32),
            jax.ShapeDtypeStruct((np_, nc + np_), F32),
        ),
        in_specs=[pl.BlockSpec(memory_space=pltpu.HBM)] * 3,
        out_specs=(vmem,) * 4,
        scratch_shapes=scratch,
        compiler_params=pltpu.CompilerParams(collective_id=0, has_side_effects=True, vmem_limit_bytes=48 << 20),
        cost_estimate=pl.CostEstimate(flops=10**9, bytes_accessed=4 << 20, transcendentals=0),
    )(*[pltpu.with_memory_space_constraint(v, pltpu.HBM) for v in (basis, panel, rate_codes)])
    return (q1, q2, c1.T, c2.T)


def solution(mesh):
    nx = 4
    nz = mesh.shape["gx"] // nx
    ny = mesh.shape["gy"] // 2
    placed = P(None, "gx", "gy")
    return jax.shard_map(
        functools.partial(local, nz, nx, ny),
        mesh=mesh,
        in_specs=(placed, placed, placed),
        out_specs=(placed, placed, P(), P()),
        check_vma=False,
    )
```

```python
import functools

import jax
import jax.numpy as jnp
from jax import lax
from jax.experimental import pallas as pl
from jax.experimental.pallas import tpu as pltpu
from jax.sharding import PartitionSpec as P

HIGH = lax.Precision.HIGHEST
MESH = pl.DeviceIdType.MESH
F32 = jnp.float32
BF16 = jnp.bfloat16
NN = (((1,), (0,)), ((), ()))
NT = (((1,), (1,)), ((), ()))
LANES = 128


def small_dot(a, b, dims):
    return lax.dot_general(a, b, dims, precision=HIGH, preferred_element_type=F32)


def split_two(x):
    hi = x.astype(BF16)
    lo = (x - hi.astype(F32)).astype(BF16)
    return hi, lo


def eliminate(gram):
    n = gram.shape[0]
    row = lax.broadcasted_iota(jnp.int32, (n, n), 0)
    col = lax.broadcasted_iota(jnp.int32, (n, n), 1)
    left = gram
    right = jnp.where(row == col, 1.0, 0.0).astype(F32)
    for j in range(n):
        factor = jnp.where(row[:, :1] > j, left[:, j : j + 1] / left[j : j + 1, j : j + 1], 0.0)
        left, right = (left - factor * left[j : j + 1, :], right - factor * right[j : j + 1, :])
    diag = jnp.sum(jnp.where(row == col, left, 0.0), axis=1, keepdims=True)
    root = 1.0 / jnp.sqrt(diag)
    return jnp.where(row <= col, left * root, 0.0), right * root


def kernel(
    dims,
    b_hbm, p_hbm, codes_hbm,
    q1_ref, q2_ref, c1_ref, c2_ref,
    xt, wt, codes, rf, up_r, dn_r, pack_l, pack_r, from_l, from_r, wpack_l, wpack_r, wfrom_l, wfrom_r,
    part, z2, acc, accw, payload, rs_buf, a_buf, b_buf, full,
    load_sem, halo_send, halo_recv, red_send, red_recv,
):
    nz, nx, ny, rows, nb, np_, scale = dims
    nm = nx * 2
    gx, gy = lax.axis_index("gx"), lax.axis_index("gy")
    zz, xx = gx // nx, gx % nx
    yy, core = gy // 2, gy % 2
    member = xx * 2 + core
    ngx, ngy = nz * nx, ny * 2
    above = ((gx + ngx - 1) % ngx, gy)
    below = ((gx + 1) % ngx, gy)
    left = (gx, (gy + ngy - 1) % ngy)
    right = (gx, (gy + 1) % ngy)

    def in_team(d):
        m = (member + d) % nm
        return (zz * nx + m // 2, yy * 2 + m % 2)

    def in_y(d):
        return (gx, ((yy + d) % ny) * 2 + core)

    def in_z(d):
        return (((zz + d) % nz) * nx + xx, gy)

    def in_first(d):
        a, b = in_y(d), in_z(d)
        return (a[0] * (1 - core) + b[0] * core, a[1] * (1 - core) + b[1] * core)

    def in_second(d):
        a, b = in_z(d), in_y(d)
        return (a[0] * (1 - core) + b[0] * core, a[1] * (1 - core) + b[1] * core)

    peers = [above, below, left, right]
    peers += [in_team(d) for d in range(1, nm)]
    peers += [in_y(d) for d in range(1, ny)]
    peers += [in_z(d) for d in range(1, nz)]
    barrier = pltpu.get_barrier_semaphore()
    for peer in peers:
        pl.semaphore_signal(barrier, inc=1, device_id=peer, device_id_type=MESH)

    nc = nb + np_
    nt = nb * 2 + np_ * 2
    inner = slice(1, rows + 1)
    load_codes = pltpu.make_async_copy(codes_hbm, codes, load_sem.at[0])
    load_codes.start()
    for c in range(np_):
        pltpu.make_async_copy(p_hbm.at[c], xt.at[inner, nb + c], load_sem.at[1]).start()
    for c in range(nb):
        pltpu.make_async_copy(b_hbm.at[c], xt.at[inner, c], load_sem.at[2]).start()

    lane = lax.broadcasted_iota(jnp.int32, (1, LANES), 1)
    top = 8

    def rate(d, r):
        return rf[d, pl.ds(r + top, 1), :]

    def pack_step(x, r, accs):
        y = jnp.where(lane == LANES - 1, rate(3, r) * x, rate(2, r) * x)
        y = pltpu.roll(y, 2 * r, 1)
        a, b = accs
        return (jnp.where(lane == 2 * r, y, a), jnp.where(lane == (2 * r + LANES - 1) % LANES, y, b))

    def pack(at, n):
        per = 8

        def body(k, accs):
            for i in range(per):
                accs = pack_step(xt[k * per + i + 1, at], k * per + i, accs)
            return accs

        zero = jnp.zeros((n, LANES), F32)
        a, b = lax.fori_loop(0, rows // per, body, (zero, zero))
        pack_l[at] = a
        pack_r[at] = b

    load_codes.wait()
    values = codes[...].astype(F32) * 0.125
    rf[0:4, top : top + rows] = values
    rf[4, top : top + rows] = values[0] + values[1] + values[2] + values[3]
    pltpu.make_async_copy(p_hbm, xt.at[inner, nb:nc], load_sem.at[1]).wait()
    pack(slice(nb, nc), np_)

    pl.semaphore_wait(barrier, len(peers))

    def halo(k, src, dst, peer):
        c = pltpu.make_async_remote_copy(
            src_ref=src, dst_ref=dst, send_sem=halo_send.at[k], recv_sem=halo_recv.at[k],
            device_id=peer, device_id_type=MESH,
        )
        c.start()
        return c

    small = [
        halo(0, xt.at[rows, nb:nc], xt.at[0, nb:nc], below),
        halo(1, xt.at[1, nb:nc], xt.at[rows + 1, nb:nc], above),
        halo(2, pack_r.at[nb:nc], from_l.at[nb:nc], right),
        halo(3, pack_l.at[nb:nc], from_r.at[nb:nc], left),
        halo(4, codes.at[1, rows - 8 : rows], up_r, below),
        halo(5, codes.at[0, 0:8], dn_r, above),
    ]
    pltpu.make_async_copy(b_hbm, xt.at[inner, 0:nb], load_sem.at[2]).wait()
    big = [
        halo(6, xt.at[rows, 0:nb], xt.at[0, 0:nb], below),
        halo(7, xt.at[1, 0:nb], xt.at[rows + 1, 0:nb], above),
    ]
    pack(slice(0, nb), nb)
    big += [
        halo(8, pack_r.at[0:nb], from_l.at[0:nb], right),
        halo(9, pack_l.at[0:nb], from_r.at[0:nb], left),
    ]

    na, n2 = 2 * nb, 2 * np_

    def at_row(r):
        return pl.ds(pl.multiple_of(r * LANES, LANES), LANES)

    def put(first, r, x):
        hi, lo = split_two(x)
        z2[first : first + nb, at_row(r)] = hi
        z2[na + first : na + first + nb, at_row(r)] = lo

    def own(r, x):
        from_l = jnp.where(lane == 0, 0.0, pltpu.roll(rate(3, r) * x, 1, 1))
        from_r = jnp.where(lane == LANES - 1, 0.0, pltpu.roll(rate(2, r) * x, LANES - 1, 1))
        return from_l + from_r - rate(4, r) * x

    def other(r, xu, xd, sides):
        side = pltpu.roll(sides, (2 * LANES - 1 - 2 * r) % LANES, 1)
        return rate(1, r - 1) * xu + rate(0, r + 1) * xd + jnp.where((lane == 0) | (lane == LANES - 1), side, 0.0)

    def own_step(k, _):
        for i in range(4):
            r = 4 * k + i
            x = xt[r + 1, 0:nb]
            put(0, r, x)
            part[r] = own(r, x)
        return 0

    lax.fori_loop(0, rows // 4, own_step, 0)

    def sweep(x_at, sides, emit, carry, per):
        def body(k, c):
            rs = [k * per + i for i in range(per)]
            outs = [own(r, x_at(r)) + other(r, x_at(r - 1), x_at(r + 1), sides) for r in rs]
            for r, out in zip(rs, outs):
                c = emit(r, out, c)
            return c

        return lax.fori_loop(0, rows // per, body, carry)

    def both_sides(fl, fr):
        return jnp.where(lane % 2 == 0, fr * has_r, pltpu.roll(fl, 2, 1) * has_l)

    def present(k):
        return jnp.where(k, 1.0, 0.0).astype(F32)

    has_l, has_r = present(gy > 0), present(gy < ngy - 1)
    for c in small:
        c.wait()
    rf[1, top - 1 : top] = up_r[7:8].astype(F32) * 0.125 * present(gx > 0)
    rf[0, top + rows : top + rows + 1] = dn_r[0:1].astype(F32) * 0.125 * present(gx < ngx - 1)

    def emit_w(r, out, accs):
        wt[r + 1] = out
        return pack_step(out, r, accs)

    zp = jnp.zeros((np_, LANES), F32)
    a, b = sweep(lambda r: xt[r + 1, nb:nc], both_sides(from_l[nb:nc], from_r[nb:nc]), emit_w, (zp, zp), 16)
    wpack_l[...] = a
    wpack_r[...] = b
    wsend = [
        halo(10, wt.at[rows], wt.at[0], below),
        halo(11, wt.at[1], wt.at[rows + 1], above),
        halo(12, wpack_r, wfrom_l, right),
        halo(13, wpack_l, wfrom_r, left),
    ]

    for c in big:
        c.wait()

    sides_b = both_sides(from_l[0:nb], from_r[0:nb])

    def other_step(k, _):
        for i in range(4):
            r = 4 * k + i
            put(nb, r, part[r] + other(r, xt[r, 0:nb], xt[r + 2, 0:nb], sides_b))
        return 0

    lax.fori_loop(0, rows // 4, other_step, 0)

    end = rows * LANES
    step = min(2048, end)
    acc[...] = jnp.zeros_like(acc)

    def gram_step(k, _):
        at = pl.ds(pl.multiple_of(k * step, step), step)
        acc[...] += lax.dot_general(z2[0 : 2 * na, at], z2[0:na, at], NT, preferred_element_type=F32)
        return 0

    lax.fori_loop(0, end // step, gram_step, 0)

    for c in wsend:
        c.wait()

    def emit_aw(r, out, c):
        x = jnp.concatenate([wt[r + 1], out], axis=0)
        hi, lo = split_two(x)
        z2[2 * na : 2 * na + n2, at_row(r)] = hi
        z2[2 * na + n2 : 2 * na + 2 * n2, at_row(r)] = lo
        z2[2 * na + 2 * n2 :, at_row(r)] = (x - hi.astype(F32) - lo.astype(F32)).astype(BF16)
        return c

    sweep(lambda r: wt[r + 1], both_sides(wfrom_l[...], wfrom_r[...]), emit_aw, 0, 16)

    accw[...] = jnp.zeros_like(accw)

    def gram_w_step(k, _):
        at = pl.ds(pl.multiple_of(k * step, step), step)
        accw[...] += lax.dot_general(
            z2[0 : 2 * na + 2 * n2, at], z2[2 * na : 2 * na + 2 * n2, at], NT, preferred_element_type=F32
        )
        return 0

    lax.fori_loop(0, end // step, gram_w_step, 0)
    aa = acc[0:na] * 0.5 + acc[na : 2 * na]
    aa = aa + aa.T
    by_w = accw[...]
    by_w = by_w[:, 0:n2] + by_w[:, n2 : 2 * n2]
    aw = by_w[0:na] + by_w[na : 2 * na]
    ww = by_w[2 * na : 2 * na + n2] + by_w[2 * na + n2 :]
    wa = jnp.concatenate([aw, jnp.zeros((na, LANES - n2), F32)], axis=1).T[0:n2]
    low = lane < nb
    site = lax.broadcasted_iota(jnp.int32, (nb, LANES), 0)
    upper, same = lane >= site, lane == site
    ab_ab = pltpu.roll(aa[nb:na], nb, 1)
    main = jnp.where(low & ~upper, ab_ab, aa[0:nb])
    diag = jnp.sum(jnp.where(same, ab_ab, 0.0), axis=0, keepdims=True)
    extra = jnp.concatenate(
        [
            wa,
            jnp.concatenate([ww[0:np_], ww[np_:n2], jnp.zeros((np_, LANES - 2 * n2), F32)], axis=1),
            jnp.broadcast_to(diag, (8, LANES)),
        ],
        axis=0,
    )
    per_main, per_extra = nb // nm, 32 // nm
    per_all = per_main + per_extra
    for m in range(nm):
        payload[m, 0:per_main] = main[m * per_main : (m + 1) * per_main]
        payload[m, per_main:per_all] = extra[m * per_extra : (m + 1) * per_extra]

    def reduce_copy(k, src, dst, peer):
        c = pltpu.make_async_remote_copy(
            src_ref=src.at[0:per_all], dst_ref=dst.at[0:per_all], send_sem=red_send.at[k], recv_sem=red_recv.at[k],
            device_id=peer, device_id_type=MESH,
        )
        c.start()
        return c

    copies = []
    for d in range(1, nm):
        copies.append(reduce_copy(d, payload.at[(member + d) % nm], rs_buf.at[member], in_team(d)))
    rs_buf[member, 0:per_all] = payload[member, 0:per_all]
    for c in copies:
        c.wait()

    def ordered_sum(buf, n):
        total = buf[0, 0:per_all]
        for i in range(1, n):
            total = total + buf[i, 0:per_all]
        return total

    one = yy * (1 - core) + zz * core
    two = zz * (1 - core) + yy * core
    a_buf[one, 0:per_all] = ordered_sum(rs_buf, nm)
    copies = [reduce_copy(nm + d, a_buf.at[one], a_buf.at[one], in_first(d)) for d in range(1, ny)]
    for c in copies:
        c.wait()
    b_buf[two, 0:per_all] = ordered_sum(a_buf, ny)
    copies = [reduce_copy(nm + ny + d, b_buf.at[two], b_buf.at[two], in_second(d)) for d in range(1, nz)]
    for c in copies:
        c.wait()
    full[member, 0:per_all] = ordered_sum(b_buf, nz)
    copies = [
        reduce_copy(nm + ny + nz + d, full.at[member], full.at[member], in_team(d)) for d in range(1, nm)
    ]
    for c in copies:
        c.wait()

    main = jnp.concatenate([full[m, 0:per_main] for m in range(nm)], axis=0) * scale
    extra = jnp.concatenate([full[m, per_main:per_all] for m in range(nm)], axis=0) * scale
    wa = extra[0:n2]
    ww = extra[n2 : n2 + np_]
    diag = extra[n2 + np_ : n2 + np_ + 1]
    square = jnp.where(low, main, 0.0)
    flip = jnp.concatenate([square, jnp.zeros_like(square)], axis=0).T[0:nb]
    gb = jnp.where(low & ~upper, flip, main)
    ab_ab = jnp.where(low, jnp.where(upper, jnp.where(same, diag, flip), square), 0.0)
    ga_rows = jnp.concatenate([gb, pltpu.roll(ab_ab, nb, 1)], axis=0)
    w1a, w2a = wa[0:np_], wa[np_:]
    h1 = jnp.where(low, w1a, 0.0)
    v_a = w1a - small_dot(h1[:, 0:nb], gb, NN)
    v_w = ww[:, 0:n2] - small_dot(h1, wa, NT)
    gram = v_w[:, 0:np_] - small_dot(v_a, h1, NT)
    lt1, li1 = eliminate(gram)
    t_b = -small_dot(li1, h1, NN)
    t_a = small_dot(li1, v_a, NN)
    t_w = small_dot(li1, v_w, NN)
    u_a = pltpu.roll(t_b, nb, 1)
    gu_a = small_dot(u_a, ga_rows, NT) + small_dot(li1, w2a, NN)
    gu_w = small_dot(u_a, wa, NT) + small_dot(li1, ww[:, n2 : 2 * n2], NN)
    h2b = jnp.where(low, gu_a, 0.0)
    h2q = small_dot(h2b, t_b, NT) + small_dot(gu_w[:, 0:np_], li1, NT)
    c2a = u_a - h2b - small_dot(h2q, t_b, NN)
    c2w = -small_dot(h2q, li1, NN)
    g2a = gu_a - small_dot(h2b[:, 0:nb], gb, NN) - small_dot(h2q, t_a, NN)
    g2w = gu_w - small_dot(h2b, wa, NT) - small_dot(h2q, t_w, NN)
    gram = small_dot(c2a, g2a, NT) + small_dot(c2w, g2w[:, 0:np_], NT) + small_dot(li1, g2w[:, np_:], NT)
    lt2, li2 = eliminate(gram)
    d_a = small_dot(li2, c2a, NN)
    d_w = small_dot(li2, c2w, NN)
    d_v = small_dot(li2, li1, NN)
    zero = jnp.zeros((np_, np_), F32)
    coef_a = jnp.concatenate([t_b, d_a], axis=0)
    coef_w = jnp.concatenate(
        [jnp.concatenate([li1, zero], axis=1), jnp.concatenate([d_w, d_v], axis=1)], axis=0
    )
    a_hi, a_mid = split_two(coef_a)
    a_lo = (coef_a - a_hi.astype(F32) - a_mid.astype(F32)).astype(BF16)
    w_hi, w_mid = split_two(coef_w)
    w_lo = (coef_w - w_hi.astype(F32) - w_mid.astype(F32)).astype(BF16)
    a_no, w_no = jnp.zeros_like(a_lo), jnp.zeros_like(w_lo)
    three = jnp.concatenate(
        [
            jnp.concatenate([a_hi, a_hi, w_hi, w_hi, w_hi], axis=1),
            jnp.concatenate([a_mid, a_mid, w_mid, w_mid, w_no], axis=1),
            jnp.concatenate([a_lo, a_no, w_lo, w_no, w_no], axis=1),
        ],
        axis=0,
    )
    per = min(8, rows)
    width = per * LANES

    def last_step(k, _):
        at = pl.ds(pl.multiple_of(k * width, width), width)
        o = lax.dot_general(three, z2[:, at], NN, preferred_element_type=F32)
        out = o[0:n2] + (o[n2 : 2 * n2] + o[2 * n2 :])
        for i in range(per):
            q1_ref[:, k * per + i, :] = out[0:np_, i * LANES : (i + 1) * LANES]
            q2_ref[:, k * per + i, :] = out[np_:, i * LANES : (i + 1) * LANES]
        return 0

    lax.fori_loop(0, rows // per, last_step, 0)

    def placed(x, first):
        wide = jnp.concatenate([x, jnp.zeros((np_, LANES - np_), F32)], axis=1)
        return pltpu.roll(wide, first, 1)

    c1_ref[...] = (h1 + placed(lt1.T, nb))[:, 0:nc]
    c2_ref[...] = (h2b + placed(h2q, nb) + placed(lt2.T, nc))[:, 0 : nc + np_]


def local(nz, nx, ny, basis, panel, rate_codes):
    nb, rows, width = basis.shape
    np_ = panel.shape[0]
    sites = rows * width * nz * nx * ny * 2
    nc, nt, flat, nm = nb + np_, 2 * nb + 2 * np_, rows * width, nx * 2
    dims = (nz, nx, ny, rows, nb, np_, 1.0 / sites)
    vm = pltpu.VMEM
    tile = lambda *n: vm((*n, LANES), F32)
    dma = pltpu.SemaphoreType.DMA
    scratch = [
        tile(rows + 2, nc), tile(rows + 2, np_), vm((4, rows, LANES), jnp.int32), tile(5, rows + 16),
        vm((8, LANES), jnp.int32), vm((8, LANES), jnp.int32),
        tile(nc), tile(nc), tile(nc), tile(nc), tile(np_), tile(np_), tile(np_), tile(np_),
        tile(rows, nb), vm((4 * nb + 6 * np_, flat), BF16), vm((4 * nb, 2 * nb), F32), vm((2 * nt, 4 * np_), F32),
        tile(nm, 16), tile(nm, 16), tile(ny, 16), tile(nz, 16), tile(nm, 16),
        dma((3,)), dma((14,)), dma((14,)), dma((2 * nm + ny + nz,)), dma((2 * nm + ny + nz,)),
    ]
    vmem = pl.BlockSpec(memory_space=pltpu.VMEM)
    q1, q2, c1, c2 = pl.pallas_call(
        functools.partial(kernel, dims),
        out_shape=(
            jax.ShapeDtypeStruct((np_, rows, width), F32),
            jax.ShapeDtypeStruct((np_, rows, width), F32),
            jax.ShapeDtypeStruct((np_, nc), F32),
            jax.ShapeDtypeStruct((np_, nc + np_), F32),
        ),
        in_specs=[pl.BlockSpec(memory_space=pltpu.HBM)] * 3,
        out_specs=(vmem,) * 4,
        scratch_shapes=scratch,
        compiler_params=pltpu.CompilerParams(collective_id=0, has_side_effects=True, vmem_limit_bytes=48 << 20),
        cost_estimate=pl.CostEstimate(flops=10**9, bytes_accessed=4 << 20, transcendentals=0),
    )(*[pltpu.with_memory_space_constraint(v, pltpu.HBM) for v in (basis, panel, rate_codes)])
    return (q1, q2, c1.T, c2.T)


def solution(mesh):
    nx = 4
    nz = mesh.shape["gx"] // nx
    ny = mesh.shape["gy"] // 2
    placed = P(None, "gx", "gy")
    return jax.shard_map(
        functools.partial(local, nz, nx, ny),
        mesh=mesh,
        in_specs=(placed, placed, placed),
        out_specs=(placed, placed, P(), P()),
        check_vma=False,
    )
```

```python
import functools

import jax
import jax.numpy as jnp
from jax import lax
from jax.experimental import pallas as pl
from jax.experimental.pallas import tpu as pltpu
from jax.sharding import PartitionSpec as P

HIGH = lax.Precision.HIGHEST
MESH = pl.DeviceIdType.MESH
F32 = jnp.float32
BF16 = jnp.bfloat16
NN = (((1,), (0,)), ((), ()))
NT = (((1,), (1,)), ((), ()))
TN = (((0,), (0,)), ((), ()))
LANES = 128


def small_dot(a, b, dims):
    return lax.dot_general(a, b, dims, precision=HIGH, preferred_element_type=F32)


def split_two(x):
    hi = x.astype(BF16)
    lo = (x - hi.astype(F32)).astype(BF16)
    return hi, lo


def columns(m):
    n = m.shape[0]
    return [jnp.broadcast_to(m[:, k : k + 1], (n, LANES)) for k in range(m.shape[1])]


def eliminate(gram):
    n = gram.shape[0]
    row = lax.broadcasted_iota(jnp.int32, (n, LANES), 0)
    lane = lax.broadcasted_iota(jnp.int32, (n, LANES), 1)
    left = columns(gram)
    right = [jnp.where(row == k, 1.0, 0.0).astype(F32) for k in range(n)]
    for j in range(n):
        factor = jnp.where(row > j, left[j] / left[j][j : j + 1], 0.0)
        left = [c - factor * c[j : j + 1] if k > j else c for k, c in enumerate(left)]
        right = [c - factor * c[j : j + 1] if k <= j else c for k, c in enumerate(right)]
    diag = sum(jnp.where(row == k, left[k], 0.0) for k in range(n))
    root = 1.0 / jnp.sqrt(diag)
    upper = sum(jnp.where((lane == k) & (row <= k), left[k], 0.0) for k in range(n)) * root
    inverse = sum(jnp.where(lane == k, right[k], 0.0) for k in range(n)) * root
    return upper[:, 0:n], inverse[:, 0:n]


def solve(gram, rhs):
    n = gram.shape[0]
    row = lax.broadcasted_iota(jnp.int32, (n, LANES), 0)
    lane = lax.broadcasted_iota(jnp.int32, (n, LANES), 1)
    left, right = columns(gram), columns(rhs)
    for j in range(n):
        factor = jnp.where(row != j, left[j] / left[j][j : j + 1], 0.0)
        left = [c - factor * c[j : j + 1] if k > j else c for k, c in enumerate(left)]
        right = [c - factor * c[j : j + 1] for c in right]
    diag = sum(jnp.where(row == k, left[k], 0.0) for k in range(n))
    out = sum(jnp.where(lane == k, right[k], 0.0) for k in range(n)) / diag
    return out[:, 0:n]


def kernel(
    dims,
    b_hbm, p_hbm, codes_hbm,
    z2, coef_ref, c1_ref, c2_ref,
    xt, wt, codes, rf, up_r, dn_r, pack_l, pack_r, from_l, from_r, wpack_l, wpack_r, wfrom_l, wfrom_r,
    part, acc, accw, payload, rs_buf, a_buf, b_buf, full,
    load_sem, halo_send, halo_recv, red_send, red_recv,
):
    nz, nx, ny, rows, nb, np_, scale = dims
    nm = nx * 2
    gx, gy = lax.axis_index("gx"), lax.axis_index("gy")
    zz, xx = gx // nx, gx % nx
    yy, core = gy // 2, gy % 2
    member = xx * 2 + core
    ngx, ngy = nz * nx, ny * 2
    above = ((gx + ngx - 1) % ngx, gy)
    below = ((gx + 1) % ngx, gy)
    left = (gx, (gy + ngy - 1) % ngy)
    right = (gx, (gy + 1) % ngy)

    def in_team(d):
        m = (member + d) % nm
        return (zz * nx + m // 2, yy * 2 + m % 2)

    def in_y(d):
        return (gx, ((yy + d) % ny) * 2 + core)

    def in_z(d):
        return (((zz + d) % nz) * nx + xx, gy)

    def in_first(d):
        a, b = in_y(d), in_z(d)
        return (a[0] * (1 - core) + b[0] * core, a[1] * (1 - core) + b[1] * core)

    def in_second(d):
        a, b = in_z(d), in_y(d)
        return (a[0] * (1 - core) + b[0] * core, a[1] * (1 - core) + b[1] * core)

    peers = [above, below, left, right]
    peers += [in_team(d) for d in range(1, nm)]
    peers += [in_y(d) for d in range(1, ny)]
    peers += [in_z(d) for d in range(1, nz)]
    barrier = pltpu.get_barrier_semaphore()
    for peer in peers:
        pl.semaphore_signal(barrier, inc=1, device_id=peer, device_id_type=MESH)

    nc = nb + np_
    nt = nb * 2 + np_ * 2
    inner = slice(1, rows + 1)
    load_codes = pltpu.make_async_copy(codes_hbm, codes, load_sem.at[0])
    load_codes.start()
    for c in range(np_):
        pltpu.make_async_copy(p_hbm.at[c], xt.at[inner, nb + c], load_sem.at[1]).start()
    for c in range(nb):
        pltpu.make_async_copy(b_hbm.at[c], xt.at[inner, c], load_sem.at[2]).start()

    lane = lax.broadcasted_iota(jnp.int32, (1, LANES), 1)
    top = 8

    def rate(d, r):
        return rf[d, pl.ds(r + top, 1), :]

    def pack_step(x, r, accs):
        y = jnp.where(lane == LANES - 1, rate(3, r) * x, rate(2, r) * x)
        y = pltpu.roll(y, 2 * r, 1)
        a, b = accs
        return (jnp.where(lane == 2 * r, y, a), jnp.where(lane == (2 * r + LANES - 1) % LANES, y, b))

    def pack(at, n):
        per = 8

        def body(k, accs):
            for i in range(per):
                accs = pack_step(xt[k * per + i + 1, at], k * per + i, accs)
            return accs

        zero = jnp.zeros((n, LANES), F32)
        a, b = lax.fori_loop(0, rows // per, body, (zero, zero))
        pack_l[at] = a
        pack_r[at] = b

    load_codes.wait()
    values = codes[...].astype(F32) * 0.125
    rf[0:4, top : top + rows] = values
    rf[4, top : top + rows] = values[0] + values[1] + values[2] + values[3]
    pltpu.make_async_copy(p_hbm, xt.at[inner, nb:nc], load_sem.at[1]).wait()
    pack(slice(nb, nc), np_)

    pl.semaphore_wait(barrier, len(peers))

    def halo(k, src, dst, peer):
        c = pltpu.make_async_remote_copy(
            src_ref=src, dst_ref=dst, send_sem=halo_send.at[k], recv_sem=halo_recv.at[k],
            device_id=peer, device_id_type=MESH,
        )
        c.start()
        return c

    small = [
        halo(0, xt.at[rows, nb:nc], xt.at[0, nb:nc], below),
        halo(1, xt.at[1, nb:nc], xt.at[rows + 1, nb:nc], above),
        halo(2, pack_r.at[nb:nc], from_l.at[nb:nc], right),
        halo(3, pack_l.at[nb:nc], from_r.at[nb:nc], left),
        halo(4, codes.at[1, rows - 8 : rows], up_r, below),
        halo(5, codes.at[0, 0:8], dn_r, above),
    ]
    pltpu.make_async_copy(b_hbm, xt.at[inner, 0:nb], load_sem.at[2]).wait()
    big = [
        halo(6, xt.at[rows, 0:nb], xt.at[0, 0:nb], below),
        halo(7, xt.at[1, 0:nb], xt.at[rows + 1, 0:nb], above),
    ]
    pack(slice(0, nb), nb)
    big += [
        halo(8, pack_r.at[0:nb], from_l.at[0:nb], right),
        halo(9, pack_l.at[0:nb], from_r.at[0:nb], left),
    ]

    na, n2 = 2 * nb, 2 * np_

    def at_row(r):
        return pl.ds(pl.multiple_of(r * LANES, LANES), LANES)

    def put(first, r, x):
        hi, lo = split_two(x)
        z2[first : first + nb, at_row(r)] = hi
        z2[na + first : na + first + nb, at_row(r)] = lo

    def own(r, x):
        from_l = jnp.where(lane == 0, 0.0, pltpu.roll(rate(3, r) * x, 1, 1))
        from_r = jnp.where(lane == LANES - 1, 0.0, pltpu.roll(rate(2, r) * x, LANES - 1, 1))
        return from_l + from_r - rate(4, r) * x

    def other(r, xu, xd, sides):
        side = pltpu.roll(sides, (2 * LANES - 1 - 2 * r) % LANES, 1)
        return rate(1, r - 1) * xu + rate(0, r + 1) * xd + jnp.where((lane == 0) | (lane == LANES - 1), side, 0.0)

    def own_step(k, _):
        for i in range(4):
            r = 4 * k + i
            x = xt[r + 1, 0:nb]
            put(0, r, x)
            part[r] = own(r, x)
        return 0

    lax.fori_loop(0, rows // 4, own_step, 0)

    def sweep(x_at, sides, emit, carry, per):
        def body(k, c):
            rs = [k * per + i for i in range(per)]
            outs = [own(r, x_at(r)) + other(r, x_at(r - 1), x_at(r + 1), sides) for r in rs]
            for r, out in zip(rs, outs):
                c = emit(r, out, c)
            return c

        return lax.fori_loop(0, rows // per, body, carry)

    def both_sides(fl, fr):
        return jnp.where(lane % 2 == 0, fr * has_r, pltpu.roll(fl, 2, 1) * has_l)

    def present(k):
        return jnp.where(k, 1.0, 0.0).astype(F32)

    has_l, has_r = present(gy > 0), present(gy < ngy - 1)
    for c in small:
        c.wait()
    rf[1, top - 1 : top] = up_r[7:8].astype(F32) * 0.125 * present(gx > 0)
    rf[0, top + rows : top + rows + 1] = dn_r[0:1].astype(F32) * 0.125 * present(gx < ngx - 1)

    def emit_w(r, out, accs):
        wt[r + 1] = out
        return pack_step(out, r, accs)

    zp = jnp.zeros((np_, LANES), F32)
    a, b = sweep(lambda r: xt[r + 1, nb:nc], both_sides(from_l[nb:nc], from_r[nb:nc]), emit_w, (zp, zp), 16)
    wpack_l[...] = a
    wpack_r[...] = b
    wsend = [
        halo(10, wt.at[rows], wt.at[0], below),
        halo(11, wt.at[1], wt.at[rows + 1], above),
        halo(12, wpack_r, wfrom_l, right),
        halo(13, wpack_l, wfrom_r, left),
    ]

    for c in big:
        c.wait()

    sides_b = both_sides(from_l[0:nb], from_r[0:nb])

    def other_step(k, _):
        for i in range(4):
            r = 4 * k + i
            put(nb, r, part[r] + other(r, xt[r, 0:nb], xt[r + 2, 0:nb], sides_b))
        return 0

    lax.fori_loop(0, rows // 4, other_step, 0)

    end = rows * LANES
    step = min(2048, end)
    acc[...] = jnp.zeros_like(acc)

    def gram_step(k, _):
        at = pl.ds(pl.multiple_of(k * step, step), step)
        acc[...] += lax.dot_general(z2[0 : 2 * na, at], z2[0:na, at], NT, preferred_element_type=F32)
        return 0

    lax.fori_loop(0, end // step, gram_step, 0)

    for c in wsend:
        c.wait()

    def emit_aw(r, out, c):
        x = jnp.concatenate([wt[r + 1], out], axis=0)
        hi, lo = split_two(x)
        z2[2 * na : 2 * na + n2, at_row(r)] = hi
        z2[2 * na + n2 : 2 * na + 2 * n2, at_row(r)] = lo
        z2[2 * na + 2 * n2 :, at_row(r)] = (x - hi.astype(F32) - lo.astype(F32)).astype(BF16)
        return c

    sweep(lambda r: wt[r + 1], both_sides(wfrom_l[...], wfrom_r[...]), emit_aw, 0, 16)

    accw[...] = jnp.zeros_like(accw)

    def gram_w_step(k, _):
        at = pl.ds(pl.multiple_of(k * step, step), step)
        accw[...] += lax.dot_general(
            z2[0 : 2 * na + 2 * n2, at], z2[2 * na : 2 * na + 2 * n2, at], NT, preferred_element_type=F32
        )
        return 0

    lax.fori_loop(0, end // step, gram_w_step, 0)
    aa = acc[0:na] * 0.5 + acc[na : 2 * na]
    aa = aa + aa.T
    by_w = accw[...]
    by_w = by_w[:, 0:n2] + by_w[:, n2 : 2 * n2]
    aw = by_w[0:na] + by_w[na : 2 * na]
    ww = by_w[2 * na : 2 * na + n2] + by_w[2 * na + n2 :]
    wa = jnp.concatenate([aw, jnp.zeros((na, LANES - n2), F32)], axis=1).T[0:n2]
    low = lane < nb
    site = lax.broadcasted_iota(jnp.int32, (nb, LANES), 0)
    upper, same = lane >= site, lane == site
    ab_ab = pltpu.roll(aa[nb:na], nb, 1)
    main = jnp.where(low & ~upper, ab_ab, aa[0:nb])
    diag = jnp.sum(jnp.where(same, ab_ab, 0.0), axis=0, keepdims=True)
    extra = jnp.concatenate(
        [
            wa,
            jnp.concatenate([ww[0:np_], ww[np_:n2], jnp.zeros((np_, LANES - 2 * n2), F32)], axis=1),
            jnp.broadcast_to(diag, (8, LANES)),
        ],
        axis=0,
    )
    per_main, per_extra = nb // nm, 32 // nm
    per_all = per_main + per_extra
    for m in range(nm):
        payload[m, 0:per_main] = main[m * per_main : (m + 1) * per_main]
        payload[m, per_main:per_all] = extra[m * per_extra : (m + 1) * per_extra]

    def reduce_copy(k, src, dst, peer):
        c = pltpu.make_async_remote_copy(
            src_ref=src.at[0:per_all], dst_ref=dst.at[0:per_all], send_sem=red_send.at[k], recv_sem=red_recv.at[k],
            device_id=peer, device_id_type=MESH,
        )
        c.start()
        return c

    copies = []
    for d in range(1, nm):
        copies.append(reduce_copy(d, payload.at[(member + d) % nm], rs_buf.at[member], in_team(d)))
    rs_buf[member, 0:per_all] = payload[member, 0:per_all]
    for c in copies:
        c.wait()

    def ordered_sum(buf, n):
        total = buf[0, 0:per_all]
        for i in range(1, n):
            total = total + buf[i, 0:per_all]
        return total

    one = yy * (1 - core) + zz * core
    two = zz * (1 - core) + yy * core
    a_buf[one, 0:per_all] = ordered_sum(rs_buf, nm)
    copies = [reduce_copy(nm + d, a_buf.at[one], a_buf.at[one], in_first(d)) for d in range(1, ny)]
    for c in copies:
        c.wait()
    b_buf[two, 0:per_all] = ordered_sum(a_buf, ny)
    copies = [reduce_copy(nm + ny + d, b_buf.at[two], b_buf.at[two], in_second(d)) for d in range(1, nz)]
    for c in copies:
        c.wait()
    full[member, 0:per_all] = ordered_sum(b_buf, nz)
    copies = [
        reduce_copy(nm + ny + nz + d, full.at[member], full.at[member], in_team(d)) for d in range(1, nm)
    ]
    for c in copies:
        c.wait()

    main = jnp.concatenate([full[m, 0:per_main] for m in range(nm)], axis=0) * scale
    extra = jnp.concatenate([full[m, per_main:per_all] for m in range(nm)], axis=0) * scale
    wa = extra[0:n2]
    ww = extra[n2 : n2 + np_]
    diag = extra[n2 + np_ : n2 + np_ + 1]
    square = jnp.where(low, main, 0.0)
    flip = jnp.concatenate([square, jnp.zeros_like(square)], axis=0).T[0:nb]
    gb = jnp.where(low & ~upper, flip, main)
    ab_ab = jnp.where(low, jnp.where(upper, jnp.where(same, diag, flip), square), 0.0)
    ga_rows = jnp.concatenate([gb, pltpu.roll(ab_ab, nb, 1)], axis=0)
    w1a, w2a = wa[0:np_], wa[np_:]
    h1 = jnp.where(low, w1a, 0.0)
    h1_a = pltpu.roll(h1, nb, 1)
    n_a = w1a - small_dot(h1[:, 0:nb], gb, NN)
    n_w = ww[:, 0:n2] - small_dot(h1, wa, NT)
    an_a = w2a - small_dot(h1_a, ga_rows, NT)
    an_w = ww[:, n2 : 2 * n2] - small_dot(h1_a, wa, NT)
    hb = jnp.where(low, an_a, 0.0)
    gram = n_w[:, 0:np_] - small_dot(n_a, h1, NT)
    cross = ww[:, np_:n2] - small_dot(w1a, h1_a, NT) - small_dot(h1, hb, NT)
    y = solve(gram, cross)
    lt1, li1 = eliminate(gram)
    c2a = small_dot(y, h1, TN) - h1_a - hb
    g2a = an_a - small_dot(hb[:, 0:nb], gb, NN) - small_dot(y, n_a, TN)
    g2w = an_w - small_dot(hb, wa, NT) - small_dot(y, n_w, TN)
    gram = small_dot(g2a, c2a, NT) - small_dot(g2w[:, 0:np_], y, NN) + g2w[:, np_:]
    lt2, li2 = eliminate(gram)
    h2b = small_dot(li1, hb, NN)
    h2q = small_dot(small_dot(li1, cross, NT), li1, NT)
    low2 = small_dot(li1, lt2, NT)
    coef_a = jnp.concatenate([-small_dot(li1, h1, NN), small_dot(li2, c2a, NN)], axis=0)
    coef_w = jnp.concatenate(
        [
            jnp.concatenate([li1, jnp.zeros((np_, np_), F32)], axis=1),
            jnp.concatenate([-small_dot(li2, y, NT), li2], axis=1),
        ],
        axis=0,
    )
    a_hi, a_mid = split_two(coef_a)
    w_hi, w_mid = split_two(coef_w)
    coef_ref[...] = jnp.concatenate(
        [
            jnp.concatenate([a_hi, a_hi, w_hi, w_hi, w_hi], axis=1),
            jnp.concatenate([a_mid, a_mid, w_mid, w_mid, jnp.zeros_like(w_mid)], axis=1),
        ],
        axis=0,
    )

    def placed(x, first):
        wide = jnp.concatenate([x, jnp.zeros((np_, LANES - np_), F32)], axis=1)
        return pltpu.roll(wide, first, 1)

    c1_ref[...] = (h1 + placed(lt1.T, nb))[:, 0:nc]
    c2_ref[...] = (h2b + placed(h2q, nb) + placed(low2, nc))[:, 0 : nc + np_]


def product(per, np_, z2, coef_ref, c1_ref, c2_ref, q1_ref, q2_ref, o1_ref, o2_ref):
    n2 = 2 * np_
    width = per * LANES
    at = pl.ds(pl.multiple_of(pl.program_id(0) * width, width), width)
    o = lax.dot_general(coef_ref[...], z2[:, at], NN, preferred_element_type=F32)
    out = o[0:n2] + o[n2:]
    for i in range(per):
        q1_ref[:, i, :] = out[0:np_, i * LANES : (i + 1) * LANES]
        q2_ref[:, i, :] = out[np_:, i * LANES : (i + 1) * LANES]
    o1_ref[...] = c1_ref[...]
    o2_ref[...] = c2_ref[...]


def local(nz, nx, ny, basis, panel, rate_codes):
    nb, rows, width = basis.shape
    np_ = panel.shape[0]
    sites = rows * width * nz * nx * ny * 2
    nc, nt, flat, nm = nb + np_, 2 * nb + 2 * np_, rows * width, nx * 2
    dims = (nz, nx, ny, rows, nb, np_, 1.0 / sites)
    vm = pltpu.VMEM
    tile = lambda *n: vm((*n, LANES), F32)
    dma = pltpu.SemaphoreType.DMA
    scratch = [
        tile(rows + 2, nc), tile(rows + 2, np_), vm((4, rows, LANES), jnp.int32), tile(5, rows + 16),
        vm((8, LANES), jnp.int32), vm((8, LANES), jnp.int32),
        tile(nc), tile(nc), tile(nc), tile(nc), tile(np_), tile(np_), tile(np_), tile(np_),
        tile(rows, nb), vm((4 * nb, 2 * nb), F32), vm((2 * nt, 4 * np_), F32),
        tile(nm, 16), tile(nm, 16), tile(ny, 16), tile(nz, 16), tile(nm, 16),
        dma((3,)), dma((14,)), dma((14,)), dma((2 * nm + ny + nz,)), dma((2 * nm + ny + nz,)),
    ]
    vmem = pl.BlockSpec(memory_space=pltpu.VMEM)
    nz2 = 4 * nb + 6 * np_
    held = pl.pallas_call(
        functools.partial(kernel, dims),
        out_shape=(
            jax.ShapeDtypeStruct((nz2, flat), BF16),
            jax.ShapeDtypeStruct((4 * np_, nz2), BF16),
            jax.ShapeDtypeStruct((np_, nc), F32),
            jax.ShapeDtypeStruct((np_, nc + np_), F32),
        ),
        in_specs=[pl.BlockSpec(memory_space=pltpu.HBM)] * 3,
        out_specs=(vmem,) * 4,
        scratch_shapes=scratch,
        compiler_params=pltpu.CompilerParams(collective_id=0, has_side_effects=True, vmem_limit_bytes=24 << 20),
        cost_estimate=pl.CostEstimate(flops=10**9, bytes_accessed=4 << 20, transcendentals=0),
    )(*[pltpu.with_memory_space_constraint(v, pltpu.HBM) for v in (basis, panel, rate_codes)])
    per = min(16, rows)
    block = pl.BlockSpec((np_, per, width), lambda k: (0, k, 0))
    whole = lambda *shape: pl.BlockSpec(shape, lambda k: (0, 0))
    q1, q2, c1, c2 = pl.pallas_call(
        functools.partial(product, per, np_),
        grid=(rows // per,),
        out_shape=(
            jax.ShapeDtypeStruct((np_, rows, width), F32),
            jax.ShapeDtypeStruct((np_, rows, width), F32),
            jax.ShapeDtypeStruct((np_, nc), F32),
            jax.ShapeDtypeStruct((np_, nc + np_), F32),
        ),
        in_specs=[vmem] * 4,
        out_specs=(block, block, whole(np_, nc), whole(np_, nc + np_)),
        compiler_params=pltpu.CompilerParams(vmem_limit_bytes=16 << 20),
        cost_estimate=pl.CostEstimate(flops=10**9, bytes_accessed=4 << 20, transcendentals=0),
    )(*held)
    return (q1, q2, c1.T, c2.T)


def solution(mesh):
    nx = 4
    nz = mesh.shape["gx"] // nx
    ny = mesh.shape["gy"] // 2
    placed = P(None, "gx", "gy")
    return jax.shard_map(
        functools.partial(local, nz, nx, ny),
        mesh=mesh,
        in_specs=(placed, placed, placed),
        out_specs=(placed, placed, P(), P()),
        check_vma=False,
    )
```

```python
import functools

import jax
import jax.numpy as jnp
from jax import lax
from jax.experimental import pallas as pl
from jax.experimental.pallas import tpu as pltpu
from jax.sharding import PartitionSpec as P

HIGH = lax.Precision.HIGHEST
MESH = pl.DeviceIdType.MESH
F32 = jnp.float32
BF16 = jnp.bfloat16
NN = (((1,), (0,)), ((), ()))
NT = (((1,), (1,)), ((), ()))
TN = (((0,), (0,)), ((), ()))
LANES = 128


def small_dot(a, b, dims):
    return lax.dot_general(a, b, dims, precision=HIGH, preferred_element_type=F32)


def split_two(x):
    hi = x.astype(BF16)
    lo = (x - hi.astype(F32)).astype(BF16)
    return hi, lo


def columns(m):
    n = m.shape[0]
    return [jnp.broadcast_to(m[:, k : k + 1], (n, LANES)) for k in range(m.shape[1])]


def eliminate(gram):
    n = gram.shape[0]
    row = lax.broadcasted_iota(jnp.int32, (n, LANES), 0)
    lane = lax.broadcasted_iota(jnp.int32, (n, LANES), 1)
    left = columns(gram)
    right = [jnp.where(row == k, 1.0, 0.0).astype(F32) for k in range(n)]
    for j in range(n):
        factor = jnp.where(row > j, left[j] / left[j][j : j + 1], 0.0)
        left = [c - factor * c[j : j + 1] if k > j else c for k, c in enumerate(left)]
        right = [c - factor * c[j : j + 1] if k <= j else c for k, c in enumerate(right)]
    diag = sum(jnp.where(row == k, left[k], 0.0) for k in range(n))
    root = 1.0 / jnp.sqrt(diag)
    upper = sum(jnp.where((lane == k) & (row <= k), left[k], 0.0) for k in range(n)) * root
    inverse = sum(jnp.where(lane == k, right[k], 0.0) for k in range(n)) * root
    return upper[:, 0:n], inverse[:, 0:n]


def solve(gram, rhs):
    n = gram.shape[0]
    row = lax.broadcasted_iota(jnp.int32, (n, LANES), 0)
    lane = lax.broadcasted_iota(jnp.int32, (n, LANES), 1)
    left, right = columns(gram), columns(rhs)
    for j in range(n):
        factor = jnp.where(row != j, left[j] / left[j][j : j + 1], 0.0)
        left = [c - factor * c[j : j + 1] if k > j else c for k, c in enumerate(left)]
        right = [c - factor * c[j : j + 1] for c in right]
    diag = sum(jnp.where(row == k, left[k], 0.0) for k in range(n))
    out = sum(jnp.where(lane == k, right[k], 0.0) for k in range(n)) / diag
    return out[:, 0:n]


def kernel(
    dims,
    b_hbm, p_hbm, codes_hbm,
    z2, coef_ref, c1_ref, c2_ref,
    xt, wt, codes, rf, up_r, dn_r, pack_l, pack_r, from_l, from_r, wpack_l, wpack_r, wfrom_l, wfrom_r,
    part, acc, accw, payload, rs_buf, a_buf, b_buf, full,
    load_sem, halo_send, halo_recv, red_send, red_recv,
):
    nz, nx, ny, rows, nb, np_, scale = dims
    nm = nx * 2
    gx, gy = lax.axis_index("gx"), lax.axis_index("gy")
    zz, xx = gx // nx, gx % nx
    yy, core = gy // 2, gy % 2
    member = xx * 2 + core
    ngx, ngy = nz * nx, ny * 2
    above = ((gx + ngx - 1) % ngx, gy)
    below = ((gx + 1) % ngx, gy)
    left = (gx, (gy + ngy - 1) % ngy)
    right = (gx, (gy + 1) % ngy)

    def in_team(d):
        m = (member + d) % nm
        return (zz * nx + m // 2, yy * 2 + m % 2)

    def in_y(d):
        return (gx, ((yy + d) % ny) * 2 + core)

    def in_z(d):
        return (((zz + d) % nz) * nx + xx, gy)

    def in_first(d):
        a, b = in_y(d), in_z(d)
        return (a[0] * (1 - core) + b[0] * core, a[1] * (1 - core) + b[1] * core)

    def in_second(d):
        a, b = in_z(d), in_y(d)
        return (a[0] * (1 - core) + b[0] * core, a[1] * (1 - core) + b[1] * core)

    peers = [above, below, left, right]
    peers += [in_team(d) for d in range(1, nm)]
    peers += [in_y(d) for d in range(1, ny)]
    peers += [in_z(d) for d in range(1, nz)]
    barrier = pltpu.get_barrier_semaphore()
    for peer in peers:
        pl.semaphore_signal(barrier, inc=1, device_id=peer, device_id_type=MESH)

    nc = nb + np_
    nt = nb * 2 + np_ * 2
    inner = slice(1, rows + 1)
    load_codes = pltpu.make_async_copy(codes_hbm, codes, load_sem.at[0])
    load_codes.start()
    for c in range(np_):
        pltpu.make_async_copy(p_hbm.at[c], xt.at[inner, nb + c], load_sem.at[1]).start()
    for c in range(nb):
        pltpu.make_async_copy(b_hbm.at[c], xt.at[inner, c], load_sem.at[2]).start()

    lane = lax.broadcasted_iota(jnp.int32, (1, LANES), 1)
    top = 8

    def rate(d, r):
        return rf[d, pl.ds(r + top, 1), :]

    def pack_step(x, r, accs):
        y = jnp.where(lane == LANES - 1, rate(3, r) * x, rate(2, r) * x)
        y = pltpu.roll(y, 2 * r, 1)
        a, b = accs
        return (jnp.where(lane == 2 * r, y, a), jnp.where(lane == (2 * r + LANES - 1) % LANES, y, b))

    def pack(at, n):
        per = 8

        def body(k, accs):
            for i in range(per):
                accs = pack_step(xt[k * per + i + 1, at], k * per + i, accs)
            return accs

        zero = jnp.zeros((n, LANES), F32)
        a, b = lax.fori_loop(0, rows // per, body, (zero, zero))
        pack_l[at] = a
        pack_r[at] = b

    load_codes.wait()
    values = codes[...].astype(F32) * 0.125
    rf[0:4, top : top + rows] = values
    rf[4, top : top + rows] = values[0] + values[1] + values[2] + values[3]
    pltpu.make_async_copy(p_hbm, xt.at[inner, nb:nc], load_sem.at[1]).wait()
    pack(slice(nb, nc), np_)

    pl.semaphore_wait(barrier, len(peers))

    def halo(k, src, dst, peer):
        c = pltpu.make_async_remote_copy(
            src_ref=src, dst_ref=dst, send_sem=halo_send.at[k], recv_sem=halo_recv.at[k],
            device_id=peer, device_id_type=MESH,
        )
        c.start()
        return c

    small = [
        halo(0, xt.at[rows, nb:nc], xt.at[0, nb:nc], below),
        halo(1, xt.at[1, nb:nc], xt.at[rows + 1, nb:nc], above),
        halo(2, pack_r.at[nb:nc], from_l.at[nb:nc], right),
        halo(3, pack_l.at[nb:nc], from_r.at[nb:nc], left),
        halo(4, codes.at[1, rows - 8 : rows], up_r, below),
        halo(5, codes.at[0, 0:8], dn_r, above),
    ]
    pltpu.make_async_copy(b_hbm, xt.at[inner, 0:nb], load_sem.at[2]).wait()
    big = [
        halo(6, xt.at[rows, 0:nb], xt.at[0, 0:nb], below),
        halo(7, xt.at[1, 0:nb], xt.at[rows + 1, 0:nb], above),
    ]
    pack(slice(0, nb), nb)
    big += [
        halo(8, pack_r.at[0:nb], from_l.at[0:nb], right),
        halo(9, pack_l.at[0:nb], from_r.at[0:nb], left),
    ]

    na, n2 = 2 * nb, 2 * np_

    def at_row(r):
        return pl.ds(pl.multiple_of(r * LANES, LANES), LANES)

    def put(first, r, x):
        hi, lo = split_two(x)
        z2[first : first + nb, at_row(r)] = hi
        z2[na + first : na + first + nb, at_row(r)] = lo

    def own(r, x):
        from_l = jnp.where(lane == 0, 0.0, pltpu.roll(rate(3, r) * x, 1, 1))
        from_r = jnp.where(lane == LANES - 1, 0.0, pltpu.roll(rate(2, r) * x, LANES - 1, 1))
        return from_l + from_r - rate(4, r) * x

    def other(r, xu, xd, sides):
        side = pltpu.roll(sides, (2 * LANES - 1 - 2 * r) % LANES, 1)
        return rate(1, r - 1) * xu + rate(0, r + 1) * xd + jnp.where((lane == 0) | (lane == LANES - 1), side, 0.0)

    def own_step(k, _):
        for i in range(4):
            r = 4 * k + i
            x = xt[r + 1, 0:nb]
            put(0, r, x)
            part[r] = own(r, x)
        return 0

    lax.fori_loop(0, rows // 4, own_step, 0)

    def sweep(x_at, sides, emit, carry, per):
        def body(k, c):
            rs = [k * per + i for i in range(per)]
            outs = [own(r, x_at(r)) + other(r, x_at(r - 1), x_at(r + 1), sides) for r in rs]
            for r, out in zip(rs, outs):
                c = emit(r, out, c)
            return c

        return lax.fori_loop(0, rows // per, body, carry)

    def both_sides(fl, fr):
        return jnp.where(lane % 2 == 0, fr * has_r, pltpu.roll(fl, 2, 1) * has_l)

    def present(k):
        return jnp.where(k, 1.0, 0.0).astype(F32)

    has_l, has_r = present(gy > 0), present(gy < ngy - 1)
    for c in small:
        c.wait_recv()
    rf[1, top - 1 : top] = up_r[7:8].astype(F32) * 0.125 * present(gx > 0)
    rf[0, top + rows : top + rows + 1] = dn_r[0:1].astype(F32) * 0.125 * present(gx < ngx - 1)

    def emit_w(r, out, accs):
        wt[r + 1] = out
        return pack_step(out, r, accs)

    zp = jnp.zeros((np_, LANES), F32)
    a, b = sweep(lambda r: xt[r + 1, nb:nc], both_sides(from_l[nb:nc], from_r[nb:nc]), emit_w, (zp, zp), 16)
    wpack_l[...] = a
    wpack_r[...] = b
    wsend = [
        halo(10, wt.at[rows], wt.at[0], below),
        halo(11, wt.at[1], wt.at[rows + 1], above),
        halo(12, wpack_r, wfrom_l, right),
        halo(13, wpack_l, wfrom_r, left),
    ]

    for c in big:
        c.wait_recv()

    sides_b = both_sides(from_l[0:nb], from_r[0:nb])

    def other_step(k, _):
        for i in range(4):
            r = 4 * k + i
            put(nb, r, part[r] + other(r, xt[r, 0:nb], xt[r + 2, 0:nb], sides_b))
        return 0

    lax.fori_loop(0, rows // 4, other_step, 0)

    end = rows * LANES
    step = min(2048, end)
    acc[...] = jnp.zeros_like(acc)

    def gram_step(k, _):
        at = pl.ds(pl.multiple_of(k * step, step), step)
        acc[...] += lax.dot_general(z2[0 : 2 * na, at], z2[0:na, at], NT, preferred_element_type=F32)
        return 0

    lax.fori_loop(0, end // step, gram_step, 0)

    for c in wsend:
        c.wait_recv()

    def emit_aw(r, out, c):
        x = jnp.concatenate([wt[r + 1], out], axis=0)
        hi, lo = split_two(x)
        z2[2 * na : 2 * na + n2, at_row(r)] = hi
        z2[2 * na + n2 : 2 * na + 2 * n2, at_row(r)] = lo
        z2[2 * na + 2 * n2 :, at_row(r)] = (x - hi.astype(F32) - lo.astype(F32)).astype(BF16)
        return c

    sweep(lambda r: wt[r + 1], both_sides(wfrom_l[...], wfrom_r[...]), emit_aw, 0, 16)

    accw[...] = jnp.zeros_like(accw)

    def gram_w_step(k, _):
        at = pl.ds(pl.multiple_of(k * step, step), step)
        accw[...] += lax.dot_general(
            z2[0 : 2 * na + 2 * n2, at], z2[2 * na : 2 * na + 2 * n2, at], NT, preferred_element_type=F32
        )
        return 0

    lax.fori_loop(0, end // step, gram_w_step, 0)
    aa = acc[0:na] * 0.5 + acc[na : 2 * na]
    aa = aa + aa.T
    by_w = accw[...]
    by_w = by_w[:, 0:n2] + by_w[:, n2 : 2 * n2]
    aw = by_w[0:na] + by_w[na : 2 * na]
    ww = by_w[2 * na : 2 * na + n2] + by_w[2 * na + n2 :]
    wa = jnp.concatenate([aw, jnp.zeros((na, LANES - n2), F32)], axis=1).T[0:n2]
    low = lane < nb
    site = lax.broadcasted_iota(jnp.int32, (nb, LANES), 0)
    upper, same = lane >= site, lane == site
    ab_ab = pltpu.roll(aa[nb:na], nb, 1)
    main = jnp.where(low & ~upper, ab_ab, aa[0:nb])
    diag = jnp.sum(jnp.where(same, ab_ab, 0.0), axis=0, keepdims=True)
    extra = jnp.concatenate(
        [
            wa,
            jnp.concatenate([ww[0:np_], ww[np_:n2], jnp.zeros((np_, LANES - 2 * n2), F32)], axis=1),
            jnp.broadcast_to(diag, (8, LANES)),
        ],
        axis=0,
    )
    per_main, per_extra = nb // nm, 32 // nm
    per_all = per_main + per_extra
    for m in range(nm):
        payload[m, 0:per_main] = main[m * per_main : (m + 1) * per_main]
        payload[m, per_main:per_all] = extra[m * per_extra : (m + 1) * per_extra]

    def reduce_copy(k, src, dst, peer):
        c = pltpu.make_async_remote_copy(
            src_ref=src.at[0:per_all], dst_ref=dst.at[0:per_all], send_sem=red_send.at[k], recv_sem=red_recv.at[k],
            device_id=peer, device_id_type=MESH,
        )
        c.start()
        return c

    def far_first(n, hops):
        return sorted(range(1, n), key=lambda d: -hops(d))

    def ring(n):
        return far_first(n, lambda d: min(d, n - d))

    team = far_first(nm, lambda d: min(d, nm - d) + (d == nm // 2 + 1))

    def sent(copies):
        for c in copies:
            c.wait_send()

    def arrived(copies):
        for c in copies:
            c.wait_recv()

    copies = [reduce_copy(d, payload.at[(member + d) % nm], rs_buf.at[member], in_team(d)) for d in team]
    rs_buf[member, 0:per_all] = payload[member, 0:per_all]
    sent(small + big + wsend)
    arrived(copies)

    def ordered_sum(buf, n):
        total = buf[0, 0:per_all]
        for i in range(1, n):
            total = total + buf[i, 0:per_all]
        return total

    one = yy * (1 - core) + zz * core
    two = zz * (1 - core) + yy * core
    last = copies
    a_buf[one, 0:per_all] = ordered_sum(rs_buf, nm)
    copies = [reduce_copy(nm + d, a_buf.at[one], a_buf.at[one], in_first(d)) for d in ring(ny)]
    sent(last)
    arrived(copies)
    last = copies
    b_buf[two, 0:per_all] = ordered_sum(a_buf, ny)
    copies = [reduce_copy(nm + ny + d, b_buf.at[two], b_buf.at[two], in_second(d)) for d in ring(nz)]
    sent(last)
    arrived(copies)
    last = copies
    full[member, 0:per_all] = ordered_sum(b_buf, nz)
    copies = [reduce_copy(nm + ny + nz + d, full.at[member], full.at[member], in_team(d)) for d in team]
    sent(last)
    arrived(copies)
    last = copies

    main = jnp.concatenate([full[m, 0:per_main] for m in range(nm)], axis=0) * scale
    extra = jnp.concatenate([full[m, per_main:per_all] for m in range(nm)], axis=0) * scale
    wa = extra[0:n2]
    ww = extra[n2 : n2 + np_]
    diag = extra[n2 + np_ : n2 + np_ + 1]
    square = jnp.where(low, main, 0.0)
    flip = jnp.concatenate([square, jnp.zeros_like(square)], axis=0).T[0:nb]
    gb = jnp.where(low & ~upper, flip, main)
    ab_ab = jnp.where(low, jnp.where(upper, jnp.where(same, diag, flip), square), 0.0)
    ga_rows = jnp.concatenate([gb, pltpu.roll(ab_ab, nb, 1)], axis=0)
    w1a, w2a = wa[0:np_], wa[np_:]
    h1 = jnp.where(low, w1a, 0.0)
    h1_a = pltpu.roll(h1, nb, 1)
    n_a = w1a - small_dot(h1[:, 0:nb], gb, NN)
    n_w = ww[:, 0:n2] - small_dot(h1, wa, NT)
    an_a = w2a - small_dot(h1_a, ga_rows, NT)
    an_w = ww[:, n2 : 2 * n2] - small_dot(h1_a, wa, NT)
    hb = jnp.where(low, an_a, 0.0)
    gram = n_w[:, 0:np_] - small_dot(n_a, h1, NT)
    cross = ww[:, np_:n2] - small_dot(w1a, h1_a, NT) - small_dot(h1, hb, NT)
    y = solve(gram, cross)
    lt1, li1 = eliminate(gram)
    c2a = small_dot(y, h1, TN) - h1_a - hb
    g2a = an_a - small_dot(hb[:, 0:nb], gb, NN) - small_dot(y, n_a, TN)
    g2w = an_w - small_dot(hb, wa, NT) - small_dot(y, n_w, TN)
    gram = small_dot(g2a, c2a, NT) - small_dot(g2w[:, 0:np_], y, NN) + g2w[:, np_:]
    lt2, li2 = eliminate(gram)
    h2b = small_dot(li1, hb, NN)
    h2q = small_dot(small_dot(li1, cross, NT), li1, NT)
    low2 = small_dot(li1, lt2, NT)
    coef_a = jnp.concatenate([-small_dot(li1, h1, NN), small_dot(li2, c2a, NN)], axis=0)
    coef_w = jnp.concatenate(
        [
            jnp.concatenate([li1, jnp.zeros((np_, np_), F32)], axis=1),
            jnp.concatenate([-small_dot(li2, y, NT), li2], axis=1),
        ],
        axis=0,
    )
    a_hi, a_mid = split_two(coef_a)
    w_hi, w_mid = split_two(coef_w)
    coef_ref[...] = jnp.concatenate(
        [
            jnp.concatenate([a_hi, a_hi, w_hi, w_hi, w_hi], axis=1),
            jnp.concatenate([a_mid, a_mid, w_mid, w_mid, jnp.zeros_like(w_mid)], axis=1),
        ],
        axis=0,
    )

    def placed(x, first):
        wide = jnp.concatenate([x, jnp.zeros((np_, LANES - np_), F32)], axis=1)
        return pltpu.roll(wide, first, 1)

    sent(last)
    c1_ref[...] = (h1 + placed(lt1.T, nb))[:, 0:nc]
    c2_ref[...] = (h2b + placed(h2q, nb) + placed(low2, nc))[:, 0 : nc + np_]


def product(per, np_, z2, coef_ref, c1_ref, c2_ref, q1_ref, q2_ref, o1_ref, o2_ref):
    n2 = 2 * np_
    width = per * LANES
    at = pl.ds(pl.multiple_of(pl.program_id(0) * width, width), width)
    o = lax.dot_general(coef_ref[...], z2[:, at], NN, preferred_element_type=F32)
    out = o[0:n2] + o[n2:]
    for i in range(per):
        q1_ref[:, i, :] = out[0:np_, i * LANES : (i + 1) * LANES]
        q2_ref[:, i, :] = out[np_:, i * LANES : (i + 1) * LANES]
    o1_ref[...] = c1_ref[...]
    o2_ref[...] = c2_ref[...]


def local(nz, nx, ny, basis, panel, rate_codes):
    nb, rows, width = basis.shape
    np_ = panel.shape[0]
    sites = rows * width * nz * nx * ny * 2
    nc, nt, flat, nm = nb + np_, 2 * nb + 2 * np_, rows * width, nx * 2
    dims = (nz, nx, ny, rows, nb, np_, 1.0 / sites)
    vm = pltpu.VMEM
    tile = lambda *n: vm((*n, LANES), F32)
    dma = pltpu.SemaphoreType.DMA
    scratch = [
        tile(rows + 2, nc), tile(rows + 2, np_), vm((4, rows, LANES), jnp.int32), tile(5, rows + 16),
        vm((8, LANES), jnp.int32), vm((8, LANES), jnp.int32),
        tile(nc), tile(nc), tile(nc), tile(nc), tile(np_), tile(np_), tile(np_), tile(np_),
        tile(rows, nb), vm((4 * nb, 2 * nb), F32), vm((2 * nt, 4 * np_), F32),
        tile(nm, 16), tile(nm, 16), tile(ny, 16), tile(nz, 16), tile(nm, 16),
        dma((3,)), dma((14,)), dma((14,)), dma((2 * nm + ny + nz,)), dma((2 * nm + ny + nz,)),
    ]
    vmem = pl.BlockSpec(memory_space=pltpu.VMEM)
    nz2 = 4 * nb + 6 * np_
    held = pl.pallas_call(
        functools.partial(kernel, dims),
        out_shape=(
            jax.ShapeDtypeStruct((nz2, flat), BF16),
            jax.ShapeDtypeStruct((4 * np_, nz2), BF16),
            jax.ShapeDtypeStruct((np_, nc), F32),
            jax.ShapeDtypeStruct((np_, nc + np_), F32),
        ),
        in_specs=[pl.BlockSpec(memory_space=pltpu.HBM)] * 3,
        out_specs=(vmem,) * 4,
        scratch_shapes=scratch,
        compiler_params=pltpu.CompilerParams(collective_id=0, has_side_effects=True, vmem_limit_bytes=24 << 20),
        cost_estimate=pl.CostEstimate(flops=10**9, bytes_accessed=4 << 20, transcendentals=0),
    )(*[pltpu.with_memory_space_constraint(v, pltpu.HBM) for v in (basis, panel, rate_codes)])
    per = min(32, rows)
    block = pl.BlockSpec((np_, per, width), lambda k: (0, k, 0))
    whole = lambda *shape: pl.BlockSpec(shape, lambda k: (0, 0))
    q1, q2, c1, c2 = pl.pallas_call(
        functools.partial(product, per, np_),
        grid=(rows // per,),
        out_shape=(
            jax.ShapeDtypeStruct((np_, rows, width), F32),
            jax.ShapeDtypeStruct((np_, rows, width), F32),
            jax.ShapeDtypeStruct((np_, nc), F32),
            jax.ShapeDtypeStruct((np_, nc + np_), F32),
        ),
        in_specs=[vmem] * 4,
        out_specs=(block, block, whole(np_, nc), whole(np_, nc + np_)),
        compiler_params=pltpu.CompilerParams(vmem_limit_bytes=16 << 20),
        cost_estimate=pl.CostEstimate(flops=10**9, bytes_accessed=4 << 20, transcendentals=0),
    )(*held)
    return (q1, q2, c1.T, c2.T)


def solution(mesh):
    nx = 4
    nz = mesh.shape["gx"] // nx
    ny = mesh.shape["gy"] // 2
    placed = P(None, "gx", "gy")
    return jax.shard_map(
        functools.partial(local, nz, nx, ny),
        mesh=mesh,
        in_specs=(placed, placed, placed),
        out_specs=(placed, placed, P(), P()),
        check_vma=False,
    )
```

```python
import functools

import jax
import jax.numpy as jnp
from jax import lax
from jax.experimental import pallas as pl
from jax.experimental.pallas import tpu as pltpu
from jax.sharding import PartitionSpec as P

HIGH = lax.Precision.HIGHEST
MESH = pl.DeviceIdType.MESH
F32 = jnp.float32
BF16 = jnp.bfloat16
NN = (((1,), (0,)), ((), ()))
NT = (((1,), (1,)), ((), ()))
TN = (((0,), (0,)), ((), ()))
LANES = 128


def small_dot(a, b, dims):
    return lax.dot_general(a, b, dims, precision=HIGH, preferred_element_type=F32)


def split_two(x):
    hi = x.astype(BF16)
    lo = (x - hi.astype(F32)).astype(BF16)
    return hi, lo


def columns(m):
    n = m.shape[0]
    return [jnp.broadcast_to(m[:, k : k + 1], (n, LANES)) for k in range(m.shape[1])]


def eliminate(gram):
    n = gram.shape[0]
    row = lax.broadcasted_iota(jnp.int32, (n, LANES), 0)
    lane = lax.broadcasted_iota(jnp.int32, (n, LANES), 1)
    left = columns(gram)
    right = [jnp.where(row == k, 1.0, 0.0).astype(F32) for k in range(n)]
    for j in range(n):
        factor = jnp.where(row > j, left[j] / left[j][j : j + 1], 0.0)
        left = [c - factor * c[j : j + 1] if k > j else c for k, c in enumerate(left)]
        right = [c - factor * c[j : j + 1] if k <= j else c for k, c in enumerate(right)]
    diag = sum(jnp.where(row == k, left[k], 0.0) for k in range(n))
    root = 1.0 / jnp.sqrt(diag)
    upper = sum(jnp.where((lane == k) & (row <= k), left[k], 0.0) for k in range(n)) * root
    inverse = sum(jnp.where(lane == k, right[k], 0.0) for k in range(n)) * root
    return upper[:, 0:n], inverse[:, 0:n]


def solve(gram, rhs):
    n = gram.shape[0]
    row = lax.broadcasted_iota(jnp.int32, (n, LANES), 0)
    lane = lax.broadcasted_iota(jnp.int32, (n, LANES), 1)
    left, right = columns(gram), columns(rhs)
    for j in range(n):
        factor = jnp.where(row != j, left[j] / left[j][j : j + 1], 0.0)
        left = [c - factor * c[j : j + 1] if k > j else c for k, c in enumerate(left)]
        right = [c - factor * c[j : j + 1] for c in right]
    diag = sum(jnp.where(row == k, left[k], 0.0) for k in range(n))
    out = sum(jnp.where(lane == k, right[k], 0.0) for k in range(n)) / diag
    return out[:, 0:n]


def kernel(
    dims,
    b_hbm, p_hbm, codes_hbm,
    z2, coef_ref, c1_ref, c2_ref,
    xt, wt, codes, rf, up_r, dn_r, pack_l, pack_r, from_l, from_r, wpack_l, wpack_r, wfrom_l, wfrom_r,
    part, acc, accw, payload, rs_buf, a_buf, b_buf, full,
    load_sem, halo_send, halo_recv, red_send, red_recv,
):
    nz, nx, ny, rows, nb, np_, scale = dims
    nm = nx * 2
    gx, gy = lax.axis_index("gx"), lax.axis_index("gy")
    zz, xx = gx // nx, gx % nx
    yy, core = gy // 2, gy % 2
    member = xx * 2 + core
    ngx, ngy = nz * nx, ny * 2
    above = ((gx + ngx - 1) % ngx, gy)
    below = ((gx + 1) % ngx, gy)
    left = (gx, (gy + ngy - 1) % ngy)
    right = (gx, (gy + 1) % ngy)

    def in_team(d):
        m = (member + d) % nm
        return (zz * nx + m // 2, yy * 2 + m % 2)

    def in_y(d):
        return (gx, ((yy + d) % ny) * 2 + core)

    def in_z(d):
        return (((zz + d) % nz) * nx + xx, gy)

    def in_first(d):
        a, b = in_y(d), in_z(d)
        return (a[0] * (1 - core) + b[0] * core, a[1] * (1 - core) + b[1] * core)

    def in_second(d):
        a, b = in_z(d), in_y(d)
        return (a[0] * (1 - core) + b[0] * core, a[1] * (1 - core) + b[1] * core)

    peers = [above, below, left, right]
    peers += [in_team(d) for d in range(1, nm)]
    peers += [in_y(d) for d in range(1, ny)]
    peers += [in_z(d) for d in range(1, nz)]
    barrier = pltpu.get_barrier_semaphore()
    for peer in peers:
        pl.semaphore_signal(barrier, inc=1, device_id=peer, device_id_type=MESH)

    nc = nb + np_
    nt = nb * 2 + np_ * 2
    inner = slice(1, rows + 1)
    load_codes = pltpu.make_async_copy(codes_hbm, codes, load_sem.at[0])
    load_codes.start()
    for c in range(np_):
        pltpu.make_async_copy(p_hbm.at[c], xt.at[inner, nb + c], load_sem.at[1]).start()
    for c in range(nb):
        pltpu.make_async_copy(b_hbm.at[c], xt.at[inner, c], load_sem.at[2]).start()

    lane = lax.broadcasted_iota(jnp.int32, (1, LANES), 1)
    top = 8

    def rate(d, r):
        return rf[d, pl.ds(r + top, 1), :]

    def pack_step(x, r, accs):
        y = jnp.where(lane == LANES - 1, rate(3, r) * x, rate(2, r) * x)
        y = pltpu.roll(y, 2 * r, 1)
        a, b = accs
        return (jnp.where(lane == 2 * r, y, a), jnp.where(lane == (2 * r + LANES - 1) % LANES, y, b))

    def pack(at, n, per):
        def body(k, accs):
            for i in range(per):
                accs = pack_step(xt[k * per + i + 1, at], k * per + i, accs)
            return accs

        zero = jnp.zeros((n, LANES), F32)
        carry = (zero, zero)
        a, b = body(0, carry) if per == rows else lax.fori_loop(0, rows // per, body, carry)
        pack_l[at] = a
        pack_r[at] = b

    load_codes.wait()
    values = codes[...].astype(F32) * 0.125
    rf[0:4, top : top + rows] = values
    rf[4, top : top + rows] = values[0] + values[1] + values[2] + values[3]
    pltpu.make_async_copy(p_hbm, xt.at[inner, nb:nc], load_sem.at[1]).wait()
    pack(slice(nb, nc), np_, rows)

    pl.semaphore_wait(barrier, len(peers))

    def halo(k, src, dst, peer):
        c = pltpu.make_async_remote_copy(
            src_ref=src, dst_ref=dst, send_sem=halo_send.at[k], recv_sem=halo_recv.at[k],
            device_id=peer, device_id_type=MESH,
        )
        c.start()
        return c

    small = [
        halo(0, xt.at[rows, nb:nc], xt.at[0, nb:nc], below),
        halo(1, xt.at[1, nb:nc], xt.at[rows + 1, nb:nc], above),
        halo(2, pack_r.at[nb:nc], from_l.at[nb:nc], right),
        halo(3, pack_l.at[nb:nc], from_r.at[nb:nc], left),
        halo(4, codes.at[1, rows - 8 : rows], up_r, below),
        halo(5, codes.at[0, 0:8], dn_r, above),
    ]
    pltpu.make_async_copy(b_hbm, xt.at[inner, 0:nb], load_sem.at[2]).wait()
    big = [
        halo(6, xt.at[rows, 0:nb], xt.at[0, 0:nb], below),
        halo(7, xt.at[1, 0:nb], xt.at[rows + 1, 0:nb], above),
    ]
    pack(slice(0, nb), nb, 16)
    big += [
        halo(8, pack_r.at[0:nb], from_l.at[0:nb], right),
        halo(9, pack_l.at[0:nb], from_r.at[0:nb], left),
    ]

    na, n2 = 2 * nb, 2 * np_

    def at_row(r):
        return pl.ds(pl.multiple_of(r * LANES, LANES), LANES)

    def put(first, r, x):
        hi, lo = split_two(x)
        z2[first : first + nb, at_row(r)] = hi
        z2[na + first : na + first + nb, at_row(r)] = lo

    def own(r, x):
        from_l = jnp.where(lane == 0, 0.0, pltpu.roll(rate(3, r) * x, 1, 1))
        from_r = jnp.where(lane == LANES - 1, 0.0, pltpu.roll(rate(2, r) * x, LANES - 1, 1))
        return from_l + from_r - rate(4, r) * x

    def other(r, xu, xd, sides):
        side = pltpu.roll(sides, (2 * LANES - 1 - 2 * r) % LANES, 1)
        return rate(1, r - 1) * xu + rate(0, r + 1) * xd + jnp.where((lane == 0) | (lane == LANES - 1), side, 0.0)

    def own_step(k, _):
        for i in range(8):
            r = 8 * k + i
            x = xt[r + 1, 0:nb]
            put(0, r, x)
            part[r] = own(r, x)
        return 0

    lax.fori_loop(0, rows // 8, own_step, 0)

    def sweep(x_at, sides, emit, carry, per):
        def body(k, c):
            rs = [k * per + i for i in range(per)]
            outs = [own(r, x_at(r)) + other(r, x_at(r - 1), x_at(r + 1), sides) for r in rs]
            for r, out in zip(rs, outs):
                c = emit(r, out, c)
            return c

        return body(0, carry) if per == rows else lax.fori_loop(0, rows // per, body, carry)

    def both_sides(fl, fr):
        return jnp.where(lane % 2 == 0, fr * has_r, pltpu.roll(fl, 2, 1) * has_l)

    def present(k):
        return jnp.where(k, 1.0, 0.0).astype(F32)

    has_l, has_r = present(gy > 0), present(gy < ngy - 1)
    for c in small:
        c.wait_recv()
    rf[1, top - 1 : top] = up_r[7:8].astype(F32) * 0.125 * present(gx > 0)
    rf[0, top + rows : top + rows + 1] = dn_r[0:1].astype(F32) * 0.125 * present(gx < ngx - 1)

    def emit_w(r, out, accs):
        wt[r + 1] = out
        return pack_step(out, r, accs)

    zp = jnp.zeros((np_, LANES), F32)
    a, b = sweep(lambda r: xt[r + 1, nb:nc], both_sides(from_l[nb:nc], from_r[nb:nc]), emit_w, (zp, zp), rows)
    wpack_l[...] = a
    wpack_r[...] = b
    wsend = [
        halo(10, wt.at[rows], wt.at[0], below),
        halo(11, wt.at[1], wt.at[rows + 1], above),
        halo(12, wpack_r, wfrom_l, right),
        halo(13, wpack_l, wfrom_r, left),
    ]

    for c in big:
        c.wait_recv()

    sides_b = both_sides(from_l[0:nb], from_r[0:nb])

    def other_step(k, _):
        for i in range(8):
            r = 8 * k + i
            put(nb, r, part[r] + other(r, xt[r, 0:nb], xt[r + 2, 0:nb], sides_b))
        return 0

    lax.fori_loop(0, rows // 8, other_step, 0)

    end = rows * LANES
    step = min(2048, end)
    acc[...] = jnp.zeros_like(acc)

    def gram_step(k, _):
        at = pl.ds(pl.multiple_of(k * step, step), step)
        acc[...] += lax.dot_general(z2[0 : 2 * na, at], z2[0:na, at], NT, preferred_element_type=F32)
        return 0

    lax.fori_loop(0, end // step, gram_step, 0)

    for c in wsend:
        c.wait_recv()

    def emit_aw(r, out, c):
        x = jnp.concatenate([wt[r + 1], out], axis=0)
        hi, lo = split_two(x)
        z2[2 * na : 2 * na + n2, at_row(r)] = hi
        z2[2 * na + n2 : 2 * na + 2 * n2, at_row(r)] = lo
        z2[2 * na + 2 * n2 :, at_row(r)] = (x - hi.astype(F32) - lo.astype(F32)).astype(BF16)
        return c

    sides_w = both_sides(wfrom_l[...], wfrom_r[...])
    total_w = None
    span = 16
    for k in range(rows // span):
        for r in range(k * span, (k + 1) * span):
            emit_aw(r, own(r, wt[r + 1]) + other(r, wt[r], wt[r + 2], sides_w), 0)
        at = slice(k * span * LANES, (k + 1) * span * LANES)
        term = lax.dot_general(
            z2[0 : 2 * na + 2 * n2, at], z2[2 * na : 2 * na + 2 * n2, at], NT, preferred_element_type=F32
        )
        total_w = term if total_w is None else total_w + term
    accw[...] = total_w
    aa = acc[0:na] * 0.5 + acc[na : 2 * na]
    aa = aa + aa.T
    by_w = accw[...]
    by_w = by_w[:, 0:n2] + by_w[:, n2 : 2 * n2]
    aw = by_w[0:na] + by_w[na : 2 * na]
    ww = by_w[2 * na : 2 * na + n2] + by_w[2 * na + n2 :]
    wa = jnp.concatenate([aw, jnp.zeros((na, LANES - n2), F32)], axis=1).T[0:n2]
    low = lane < nb
    site = lax.broadcasted_iota(jnp.int32, (nb, LANES), 0)
    upper, same = lane >= site, lane == site
    ab_ab = pltpu.roll(aa[nb:na], nb, 1)
    main = jnp.where(low & ~upper, ab_ab, aa[0:nb])
    diag = jnp.sum(jnp.where(same, ab_ab, 0.0), axis=0, keepdims=True)
    extra = jnp.concatenate(
        [
            wa,
            jnp.concatenate([ww[0:np_], ww[np_:n2], jnp.zeros((np_, LANES - 2 * n2), F32)], axis=1),
            jnp.broadcast_to(diag, (8, LANES)),
        ],
        axis=0,
    )
    per_main, per_extra = nb // nm, 32 // nm
    per_all = per_main + per_extra
    for m in range(nm):
        payload[m, 0:per_main] = main[m * per_main : (m + 1) * per_main]
        payload[m, per_main:per_all] = extra[m * per_extra : (m + 1) * per_extra]

    def reduce_copy(k, src, dst, peer):
        c = pltpu.make_async_remote_copy(
            src_ref=src.at[0:per_all], dst_ref=dst.at[0:per_all], send_sem=red_send.at[k], recv_sem=red_recv.at[k],
            device_id=peer, device_id_type=MESH,
        )
        c.start()
        return c

    def far_first(n, hops):
        return sorted(range(1, n), key=lambda d: -hops(d))

    def ring(n):
        return far_first(n, lambda d: min(d, n - d))

    team = far_first(nm, lambda d: min(d, nm - d) + (d == nm // 2 + 1))

    def sent(copies):
        for c in copies:
            c.wait_send()

    def arrived(copies):
        for c in copies:
            c.wait_recv()

    copies = [reduce_copy(d, payload.at[(member + d) % nm], rs_buf.at[member], in_team(d)) for d in team]
    rs_buf[member, 0:per_all] = payload[member, 0:per_all]
    sent(small + big + wsend)
    arrived(copies)

    def ordered_sum(buf, n):
        total = buf[0, 0:per_all]
        for i in range(1, n):
            total = total + buf[i, 0:per_all]
        return total

    one = yy * (1 - core) + zz * core
    two = zz * (1 - core) + yy * core
    last = copies
    a_buf[one, 0:per_all] = ordered_sum(rs_buf, nm)
    copies = [reduce_copy(nm + d, a_buf.at[one], a_buf.at[one], in_first(d)) for d in ring(ny)]
    sent(last)
    arrived(copies)
    last = copies
    b_buf[two, 0:per_all] = ordered_sum(a_buf, ny)
    copies = [reduce_copy(nm + ny + d, b_buf.at[two], b_buf.at[two], in_second(d)) for d in ring(nz)]
    sent(last)
    arrived(copies)
    last = copies
    full[member, 0:per_all] = ordered_sum(b_buf, nz)
    copies = [reduce_copy(nm + ny + nz + d, full.at[member], full.at[member], in_team(d)) for d in team]
    sent(last)
    arrived(copies)
    last = copies

    main = jnp.concatenate([full[m, 0:per_main] for m in range(nm)], axis=0) * scale
    extra = jnp.concatenate([full[m, per_main:per_all] for m in range(nm)], axis=0) * scale
    wa = extra[0:n2]
    ww = extra[n2 : n2 + np_]
    diag = extra[n2 + np_ : n2 + np_ + 1]
    square = jnp.where(low, main, 0.0)
    flip = jnp.concatenate([square, jnp.zeros_like(square)], axis=0).T[0:nb]
    gb = jnp.where(low & ~upper, flip, main)
    ab_ab = jnp.where(low, jnp.where(upper, jnp.where(same, diag, flip), square), 0.0)
    ga_rows = jnp.concatenate([gb, pltpu.roll(ab_ab, nb, 1)], axis=0)
    w1a, w2a = wa[0:np_], wa[np_:]
    h1 = jnp.where(low, w1a, 0.0)
    h1_a = pltpu.roll(h1, nb, 1)
    n_a = w1a - small_dot(h1[:, 0:nb], gb, NN)
    n_w = ww[:, 0:n2] - small_dot(h1, wa, NT)
    an_a = w2a - small_dot(h1_a, ga_rows, NT)
    an_w = ww[:, n2 : 2 * n2] - small_dot(h1_a, wa, NT)
    hb = jnp.where(low, an_a, 0.0)
    gram = n_w[:, 0:np_] - small_dot(n_a, h1, NT)
    cross = ww[:, np_:n2] - small_dot(w1a, h1_a, NT) - small_dot(h1, hb, NT)
    y = solve(gram, cross)
    lt1, li1 = eliminate(gram)
    c2a = small_dot(y, h1, TN) - h1_a - hb
    g2a = an_a - small_dot(hb[:, 0:nb], gb, NN) - small_dot(y, n_a, TN)
    g2w = an_w - small_dot(hb, wa, NT) - small_dot(y, n_w, TN)
    gram = small_dot(g2a, c2a, NT) - small_dot(g2w[:, 0:np_], y, NN) + g2w[:, np_:]
    lt2, li2 = eliminate(gram)
    h2b = small_dot(li1, hb, NN)
    h2q = small_dot(small_dot(li1, cross, NT), li1, NT)
    low2 = small_dot(li1, lt2, NT)
    coef_a = jnp.concatenate([-small_dot(li1, h1, NN), small_dot(li2, c2a, NN)], axis=0)
    coef_w = jnp.concatenate(
        [
            jnp.concatenate([li1, jnp.zeros((np_, np_), F32)], axis=1),
            jnp.concatenate([-small_dot(li2, y, NT), li2], axis=1),
        ],
        axis=0,
    )
    a_hi, a_mid = split_two(coef_a)
    w_hi, w_mid = split_two(coef_w)
    coef_ref[...] = jnp.concatenate(
        [
            jnp.concatenate([a_hi, a_hi, w_hi, w_hi, w_hi], axis=1),
            jnp.concatenate([a_mid, a_mid, w_mid, w_mid, jnp.zeros_like(w_mid)], axis=1),
        ],
        axis=0,
    )

    def placed(x, first):
        wide = jnp.concatenate([x, jnp.zeros((np_, LANES - np_), F32)], axis=1)
        return pltpu.roll(wide, first, 1)

    sent(last)
    c1_ref[...] = (h1 + placed(lt1.T, nb))[:, 0:nc]
    c2_ref[...] = (h2b + placed(h2q, nb) + placed(low2, nc))[:, 0 : nc + np_]


def product(per, np_, z2, coef_ref, c1_ref, c2_ref, q1_ref, q2_ref, o1_ref, o2_ref):
    n2 = 2 * np_
    width = per * LANES
    at = pl.ds(pl.multiple_of(pl.program_id(0) * width, width), width)
    o = lax.dot_general(coef_ref[...], z2[:, at], NN, preferred_element_type=F32)
    out = o[0:n2] + o[n2:]
    for i in range(per):
        q1_ref[:, i, :] = out[0:np_, i * LANES : (i + 1) * LANES]
        q2_ref[:, i, :] = out[np_:, i * LANES : (i + 1) * LANES]
    o1_ref[...] = c1_ref[...]
    o2_ref[...] = c2_ref[...]


def local(nz, nx, ny, basis, panel, rate_codes):
    nb, rows, width = basis.shape
    np_ = panel.shape[0]
    sites = rows * width * nz * nx * ny * 2
    nc, nt, flat, nm = nb + np_, 2 * nb + 2 * np_, rows * width, nx * 2
    dims = (nz, nx, ny, rows, nb, np_, 1.0 / sites)
    vm = pltpu.VMEM
    tile = lambda *n: vm((*n, LANES), F32)
    dma = pltpu.SemaphoreType.DMA
    scratch = [
        tile(rows + 2, nc), tile(rows + 2, np_), vm((4, rows, LANES), jnp.int32), tile(5, rows + 16),
        vm((8, LANES), jnp.int32), vm((8, LANES), jnp.int32),
        tile(nc), tile(nc), tile(nc), tile(nc), tile(np_), tile(np_), tile(np_), tile(np_),
        tile(rows, nb), vm((4 * nb, 2 * nb), F32), vm((2 * nt, 4 * np_), F32),
        tile(nm, 16), tile(nm, 16), tile(ny, 16), tile(nz, 16), tile(nm, 16),
        dma((3,)), dma((14,)), dma((14,)), dma((2 * nm + ny + nz,)), dma((2 * nm + ny + nz,)),
    ]
    vmem = pl.BlockSpec(memory_space=pltpu.VMEM)
    nz2 = 4 * nb + 6 * np_
    held = pl.pallas_call(
        functools.partial(kernel, dims),
        out_shape=(
            jax.ShapeDtypeStruct((nz2, flat), BF16),
            jax.ShapeDtypeStruct((4 * np_, nz2), BF16),
            jax.ShapeDtypeStruct((np_, nc), F32),
            jax.ShapeDtypeStruct((np_, nc + np_), F32),
        ),
        in_specs=[pl.BlockSpec(memory_space=pltpu.HBM)] * 3,
        out_specs=(vmem,) * 4,
        scratch_shapes=scratch,
        compiler_params=pltpu.CompilerParams(collective_id=0, has_side_effects=True, vmem_limit_bytes=24 << 20),
        cost_estimate=pl.CostEstimate(flops=10**9, bytes_accessed=4 << 20, transcendentals=0),
    )(*[pltpu.with_memory_space_constraint(v, pltpu.HBM) for v in (basis, panel, rate_codes)])
    per = min(32, rows)
    block = pl.BlockSpec((np_, per, width), lambda k: (0, k, 0))
    whole = lambda *shape: pl.BlockSpec(shape, lambda k: (0, 0))
    q1, q2, c1, c2 = pl.pallas_call(
        functools.partial(product, per, np_),
        grid=(rows // per,),
        out_shape=(
            jax.ShapeDtypeStruct((np_, rows, width), F32),
            jax.ShapeDtypeStruct((np_, rows, width), F32),
            jax.ShapeDtypeStruct((np_, nc), F32),
            jax.ShapeDtypeStruct((np_, nc + np_), F32),
        ),
        in_specs=[vmem] * 4,
        out_specs=(block, block, whole(np_, nc), whole(np_, nc + np_)),
        compiler_params=pltpu.CompilerParams(vmem_limit_bytes=16 << 20),
        cost_estimate=pl.CostEstimate(flops=10**9, bytes_accessed=4 << 20, transcendentals=0),
    )(*held)
    return (q1, q2, c1.T, c2.T)


def solution(mesh):
    nx = 4
    nz = mesh.shape["gx"] // nx
    ny = mesh.shape["gy"] // 2
    placed = P(None, "gx", "gy")
    return jax.shard_map(
        functools.partial(local, nz, nx, ny),
        mesh=mesh,
        in_specs=(placed, placed, placed),
        out_specs=(placed, placed, P(), P()),
        check_vma=False,
    )
```

```python
import functools

import jax
import jax.numpy as jnp
from jax import lax
from jax.experimental import pallas as pl
from jax.experimental.pallas import tpu as pltpu
from jax.sharding import PartitionSpec as P

HIGH = lax.Precision.HIGHEST
MESH = pl.DeviceIdType.MESH
F32 = jnp.float32
BF16 = jnp.bfloat16
NN = (((1,), (0,)), ((), ()))
NT = (((1,), (1,)), ((), ()))
TN = (((0,), (0,)), ((), ()))
LANES = 128


def small_dot(a, b, dims):
    return lax.dot_general(a, b, dims, precision=HIGH, preferred_element_type=F32)


def split_two(x):
    hi = x.astype(BF16)
    lo = (x - hi.astype(F32)).astype(BF16)
    return hi, lo


def columns(m):
    n = m.shape[0]
    return [jnp.broadcast_to(m[:, k : k + 1], (n, LANES)) for k in range(m.shape[1])]


def eliminate(gram):
    n = gram.shape[0]
    row = lax.broadcasted_iota(jnp.int32, (n, LANES), 0)
    lane = lax.broadcasted_iota(jnp.int32, (n, LANES), 1)
    left = columns(gram)
    right = [jnp.where(row == k, 1.0, 0.0).astype(F32) for k in range(n)]
    for j in range(n):
        factor = jnp.where(row > j, left[j] / left[j][j : j + 1], 0.0)
        left = [c - factor * c[j : j + 1] if k > j else c for k, c in enumerate(left)]
        right = [c - factor * c[j : j + 1] if k <= j else c for k, c in enumerate(right)]
    diag = sum(jnp.where(row == k, left[k], 0.0) for k in range(n))
    root = 1.0 / jnp.sqrt(diag)
    upper = sum(jnp.where((lane == k) & (row <= k), left[k], 0.0) for k in range(n)) * root
    inverse = sum(jnp.where(lane == k, right[k], 0.0) for k in range(n)) * root
    return upper[:, 0:n], inverse[:, 0:n]


def solve(gram, rhs):
    n = gram.shape[0]
    row = lax.broadcasted_iota(jnp.int32, (n, LANES), 0)
    lane = lax.broadcasted_iota(jnp.int32, (n, LANES), 1)
    left, right = columns(gram), columns(rhs)
    for j in range(n):
        factor = jnp.where(row != j, left[j] / left[j][j : j + 1], 0.0)
        left = [c - factor * c[j : j + 1] if k > j else c for k, c in enumerate(left)]
        right = [c - factor * c[j : j + 1] for c in right]
    diag = sum(jnp.where(row == k, left[k], 0.0) for k in range(n))
    out = sum(jnp.where(lane == k, right[k], 0.0) for k in range(n)) / diag
    return out[:, 0:n]


def kernel(
    dims,
    b_hbm, p_hbm, codes_hbm,
    z2, coef_ref, c1_ref, c2_ref,
    xt, wt, codes, rf, up_r, dn_r, pack_l, pack_r, from_l, from_r, wpack_l, wpack_r, wfrom_l, wfrom_r,
    part, acc, accw, payload, rs_buf, a_buf, b_buf, full,
    load_sem, halo_send, halo_recv, red_send, red_recv,
):
    nz, nx, ny, rows, nb, np_, scale = dims
    nm = nx * 2
    gx, gy = lax.axis_index("gx"), lax.axis_index("gy")
    zz, xx = gx // nx, gx % nx
    yy, core = gy // 2, gy % 2
    member = xx * 2 + core
    ngx, ngy = nz * nx, ny * 2
    above = ((gx + ngx - 1) % ngx, gy)
    below = ((gx + 1) % ngx, gy)
    left = (gx, (gy + ngy - 1) % ngy)
    right = (gx, (gy + 1) % ngy)

    def in_team(d):
        m = (member + d) % nm
        return (zz * nx + m // 2, yy * 2 + m % 2)

    def in_y(d):
        return (gx, ((yy + d) % ny) * 2 + core)

    def in_z(d):
        return (((zz + d) % nz) * nx + xx, gy)

    def in_first(d):
        a, b = in_y(d), in_z(d)
        return (a[0] * (1 - core) + b[0] * core, a[1] * (1 - core) + b[1] * core)

    def in_second(d):
        a, b = in_z(d), in_y(d)
        return (a[0] * (1 - core) + b[0] * core, a[1] * (1 - core) + b[1] * core)

    peers = [above, below, left, right]
    peers += [in_team(d) for d in range(1, nm)]
    peers += [in_y(d) for d in range(1, ny)]
    peers += [in_z(d) for d in range(1, nz)]
    barrier = pltpu.get_barrier_semaphore()
    for peer in peers:
        pl.semaphore_signal(barrier, inc=1, device_id=peer, device_id_type=MESH)

    nc = nb + np_
    nt = nb * 2 + np_ * 2
    inner = slice(1, rows + 1)
    load_codes = pltpu.make_async_copy(codes_hbm, codes, load_sem.at[0])
    load_codes.start()
    for c in range(np_):
        pltpu.make_async_copy(p_hbm.at[c], xt.at[inner, nb + c], load_sem.at[1]).start()
    for c in range(nb):
        pltpu.make_async_copy(b_hbm.at[c], xt.at[inner, c], load_sem.at[2]).start()

    lane = lax.broadcasted_iota(jnp.int32, (1, LANES), 1)
    top = 8

    def rate(d, r):
        return rf[d, pl.ds(r + top, 1), :]

    def pack_step(x, r, accs):
        y = jnp.where(lane == LANES - 1, rate(3, r) * x, rate(2, r) * x)
        y = pltpu.roll(y, 2 * r, 1)
        a, b = accs
        return (jnp.where(lane == 2 * r, y, a), jnp.where(lane == (2 * r + LANES - 1) % LANES, y, b))

    def pack(at, n, per):
        def body(k, accs):
            for i in range(per):
                accs = pack_step(xt[k * per + i + 1, at], k * per + i, accs)
            return accs

        zero = jnp.zeros((n, LANES), F32)
        carry = (zero, zero)
        a, b = body(0, carry) if per == rows else lax.fori_loop(0, rows // per, body, carry)
        pack_l[at] = a
        pack_r[at] = b

    load_codes.wait()
    values = codes[...].astype(F32) * 0.125
    rf[0:4, top : top + rows] = values
    rf[4, top : top + rows] = values[0] + values[1] + values[2] + values[3]
    pltpu.make_async_copy(p_hbm, xt.at[inner, nb:nc], load_sem.at[1]).wait()
    pack(slice(nb, nc), np_, rows)

    pl.semaphore_wait(barrier, len(peers))

    def halo(k, src, dst, peer):
        c = pltpu.make_async_remote_copy(
            src_ref=src, dst_ref=dst, send_sem=halo_send.at[k], recv_sem=halo_recv.at[k],
            device_id=peer, device_id_type=MESH,
        )
        c.start()
        return c

    small = [
        halo(0, xt.at[rows, nb:nc], xt.at[0, nb:nc], below),
        halo(1, xt.at[1, nb:nc], xt.at[rows + 1, nb:nc], above),
        halo(2, pack_r.at[nb:nc], from_l.at[nb:nc], right),
        halo(3, pack_l.at[nb:nc], from_r.at[nb:nc], left),
        halo(4, codes.at[1, rows - 8 : rows], up_r, below),
        halo(5, codes.at[0, 0:8], dn_r, above),
    ]
    pltpu.make_async_copy(b_hbm, xt.at[inner, 0:nb], load_sem.at[2]).wait()
    big = [
        halo(6, xt.at[rows, 0:nb], xt.at[0, 0:nb], below),
        halo(7, xt.at[1, 0:nb], xt.at[rows + 1, 0:nb], above),
    ]
    pack(slice(0, nb), nb, 16)
    big += [
        halo(8, pack_r.at[0:nb], from_l.at[0:nb], right),
        halo(9, pack_l.at[0:nb], from_r.at[0:nb], left),
    ]

    na, n2 = 2 * nb, 2 * np_

    def at_row(r):
        return pl.ds(pl.multiple_of(r * LANES, LANES), LANES)

    def put(first, r, x):
        hi, lo = split_two(x)
        z2[first : first + nb, at_row(r)] = hi
        z2[na + first : na + first + nb, at_row(r)] = lo

    def own(r, x):
        from_l = jnp.where(lane == 0, 0.0, pltpu.roll(rate(3, r) * x, 1, 1))
        from_r = jnp.where(lane == LANES - 1, 0.0, pltpu.roll(rate(2, r) * x, LANES - 1, 1))
        return from_l + from_r - rate(4, r) * x

    def other(r, xu, xd, sides):
        side = pltpu.roll(sides, (2 * LANES - 1 - 2 * r) % LANES, 1)
        return rate(1, r - 1) * xu + rate(0, r + 1) * xd + jnp.where((lane == 0) | (lane == LANES - 1), side, 0.0)

    def own_step(k, _):
        for i in range(16):
            r = 16 * k + i
            x = xt[r + 1, 0:nb]
            put(0, r, x)
            part[r] = own(r, x)
        return 0

    lax.fori_loop(0, rows // 16, own_step, 0)

    def sweep(x_at, sides, emit, carry, per):
        def body(k, c):
            rs = [k * per + i for i in range(per)]
            outs = [own(r, x_at(r)) + other(r, x_at(r - 1), x_at(r + 1), sides) for r in rs]
            for r, out in zip(rs, outs):
                c = emit(r, out, c)
            return c

        return body(0, carry) if per == rows else lax.fori_loop(0, rows // per, body, carry)

    def both_sides(fl, fr):
        return jnp.where(lane % 2 == 0, fr * has_r, pltpu.roll(fl, 2, 1) * has_l)

    def present(k):
        return jnp.where(k, 1.0, 0.0).astype(F32)

    has_l, has_r = present(gy > 0), present(gy < ngy - 1)
    for c in small:
        c.wait_recv()
    rf[1, top - 1 : top] = up_r[7:8].astype(F32) * 0.125 * present(gx > 0)
    rf[0, top + rows : top + rows + 1] = dn_r[0:1].astype(F32) * 0.125 * present(gx < ngx - 1)

    def emit_w(r, out, accs):
        wt[r + 1] = out
        return pack_step(out, r, accs)

    zp = jnp.zeros((np_, LANES), F32)
    a, b = sweep(lambda r: xt[r + 1, nb:nc], both_sides(from_l[nb:nc], from_r[nb:nc]), emit_w, (zp, zp), rows)
    wpack_l[...] = a
    wpack_r[...] = b
    wsend = [
        halo(10, wt.at[rows], wt.at[0], below),
        halo(11, wt.at[1], wt.at[rows + 1], above),
        halo(12, wpack_r, wfrom_l, right),
        halo(13, wpack_l, wfrom_r, left),
    ]

    for c in big:
        c.wait_recv()

    sides_b = both_sides(from_l[0:nb], from_r[0:nb])

    def other_step(k, _):
        for i in range(16):
            r = 16 * k + i
            put(nb, r, part[r] + other(r, xt[r, 0:nb], xt[r + 2, 0:nb], sides_b))
        return 0

    lax.fori_loop(0, rows // 16, other_step, 0)

    end = rows * LANES
    step = min(2048, end)
    acc[...] = jnp.zeros_like(acc)

    def gram_step(k, _):
        at = pl.ds(pl.multiple_of(k * step, step), step)
        acc[...] += lax.dot_general(z2[0 : 2 * na, at], z2[0:na, at], NT, preferred_element_type=F32)
        return 0

    lax.fori_loop(0, end // step, gram_step, 0)

    for c in wsend:
        c.wait_recv()

    def emit_aw(r, out, c):
        x = jnp.concatenate([wt[r + 1], out], axis=0)
        hi, lo = split_two(x)
        z2[2 * na : 2 * na + n2, at_row(r)] = hi
        z2[2 * na + n2 : 2 * na + 2 * n2, at_row(r)] = lo
        z2[2 * na + 2 * n2 :, at_row(r)] = (x - hi.astype(F32) - lo.astype(F32)).astype(BF16)
        return c

    sides_w = both_sides(wfrom_l[...], wfrom_r[...])
    total_w = None
    span = 16
    for k in range(rows // span):
        for r in range(k * span, (k + 1) * span):
            emit_aw(r, own(r, wt[r + 1]) + other(r, wt[r], wt[r + 2], sides_w), 0)
        at = slice(k * span * LANES, (k + 1) * span * LANES)
        term = lax.dot_general(
            z2[0 : 2 * na + 2 * n2, at], z2[2 * na : 2 * na + 2 * n2, at], NT, preferred_element_type=F32
        )
        total_w = term if total_w is None else total_w + term
    accw[...] = total_w
    aa = acc[0:na] * 0.5 + acc[na : 2 * na]
    aa = aa + aa.T
    by_w = accw[...]
    by_w = by_w[:, 0:n2] + by_w[:, n2 : 2 * n2]
    aw = by_w[0:na] + by_w[na : 2 * na]
    ww = by_w[2 * na : 2 * na + n2] + by_w[2 * na + n2 :]
    wa = jnp.concatenate([aw, jnp.zeros((na, LANES - n2), F32)], axis=1).T[0:n2]
    low = lane < nb
    site = lax.broadcasted_iota(jnp.int32, (nb, LANES), 0)
    upper, same = lane >= site, lane == site
    ab_ab = pltpu.roll(aa[nb:na], nb, 1)
    main = jnp.where(low & ~upper, ab_ab, aa[0:nb])
    diag = jnp.sum(jnp.where(same, ab_ab, 0.0), axis=0, keepdims=True)
    extra = jnp.concatenate(
        [
            wa,
            jnp.concatenate([ww[0:np_], ww[np_:n2], jnp.zeros((np_, LANES - 2 * n2), F32)], axis=1),
            jnp.broadcast_to(diag, (8, LANES)),
        ],
        axis=0,
    )
    per_main, per_extra = nb // nm, 32 // nm
    per_all = per_main + per_extra
    for m in range(nm):
        payload[m, 0:per_main] = main[m * per_main : (m + 1) * per_main]
        payload[m, per_main:per_all] = extra[m * per_extra : (m + 1) * per_extra]

    def reduce_copy(k, src, dst, peer):
        c = pltpu.make_async_remote_copy(
            src_ref=src.at[0:per_all], dst_ref=dst.at[0:per_all], send_sem=red_send.at[k], recv_sem=red_recv.at[k],
            device_id=peer, device_id_type=MESH,
        )
        c.start()
        return c

    def far_first(n, hops):
        return sorted(range(1, n), key=lambda d: -hops(d))

    def ring(n):
        return far_first(n, lambda d: min(d, n - d))

    team = far_first(nm, lambda d: min(d, nm - d) + (d == nm // 2 + 1))

    def sent(copies):
        for c in copies:
            c.wait_send()

    def arrived(copies):
        for c in copies:
            c.wait_recv()

    copies = [reduce_copy(d, payload.at[(member + d) % nm], rs_buf.at[member], in_team(d)) for d in team]
    rs_buf[member, 0:per_all] = payload[member, 0:per_all]
    sent(small + big + wsend)
    arrived(copies)

    def ordered_sum(buf, n):
        total = buf[0, 0:per_all]
        for i in range(1, n):
            total = total + buf[i, 0:per_all]
        return total

    one = yy * (1 - core) + zz * core
    two = zz * (1 - core) + yy * core
    last = copies
    a_buf[one, 0:per_all] = ordered_sum(rs_buf, nm)
    copies = [reduce_copy(nm + d, a_buf.at[one], a_buf.at[one], in_first(d)) for d in ring(ny)]
    sent(last)
    arrived(copies)
    last = copies
    b_buf[two, 0:per_all] = ordered_sum(a_buf, ny)
    copies = [reduce_copy(nm + ny + d, b_buf.at[two], b_buf.at[two], in_second(d)) for d in ring(nz)]
    sent(last)
    arrived(copies)
    last = copies
    full[member, 0:per_all] = ordered_sum(b_buf, nz)
    copies = [reduce_copy(nm + ny + nz + d, full.at[member], full.at[member], in_team(d)) for d in team]
    sent(last)
    arrived(copies)
    last = copies

    main = jnp.concatenate([full[m, 0:per_main] for m in range(nm)], axis=0) * scale
    extra = jnp.concatenate([full[m, per_main:per_all] for m in range(nm)], axis=0) * scale
    wa = extra[0:n2]
    ww = extra[n2 : n2 + np_]
    diag = extra[n2 + np_ : n2 + np_ + 1]
    square = jnp.where(low, main, 0.0)
    flip = jnp.concatenate([square, jnp.zeros_like(square)], axis=0).T[0:nb]
    gb = jnp.where(low & ~upper, flip, main)
    ab_ab = jnp.where(low, jnp.where(upper, jnp.where(same, diag, flip), square), 0.0)
    ga_rows = jnp.concatenate([gb, pltpu.roll(ab_ab, nb, 1)], axis=0)
    w1a, w2a = wa[0:np_], wa[np_:]
    h1 = jnp.where(low, w1a, 0.0)
    h1_a = pltpu.roll(h1, nb, 1)
    n_a = w1a - small_dot(h1[:, 0:nb], gb, NN)
    n_w = ww[:, 0:n2] - small_dot(h1, wa, NT)
    an_a = w2a - small_dot(h1_a, ga_rows, NT)
    an_w = ww[:, n2 : 2 * n2] - small_dot(h1_a, wa, NT)
    hb = jnp.where(low, an_a, 0.0)
    gram = n_w[:, 0:np_] - small_dot(n_a, h1, NT)
    cross = ww[:, np_:n2] - small_dot(w1a, h1_a, NT) - small_dot(h1, hb, NT)
    y = solve(gram, cross)
    lt1, li1 = eliminate(gram)
    c2a = small_dot(y, h1, TN) - h1_a - hb
    g2a = an_a - small_dot(hb[:, 0:nb], gb, NN) - small_dot(y, n_a, TN)
    g2w = an_w - small_dot(hb, wa, NT) - small_dot(y, n_w, TN)
    gram = small_dot(g2a, c2a, NT) - small_dot(g2w[:, 0:np_], y, NN) + g2w[:, np_:]
    lt2, li2 = eliminate(gram)
    h2b = small_dot(li1, hb, NN)
    h2q = small_dot(small_dot(li1, cross, NT), li1, NT)
    low2 = small_dot(li1, lt2, NT)
    coef_a = jnp.concatenate([-small_dot(li1, h1, NN), small_dot(li2, c2a, NN)], axis=0)
    coef_w = jnp.concatenate(
        [
            jnp.concatenate([li1, jnp.zeros((np_, np_), F32)], axis=1),
            jnp.concatenate([-small_dot(li2, y, NT), li2], axis=1),
        ],
        axis=0,
    )
    a_hi, a_mid = split_two(coef_a)
    w_hi, w_mid = split_two(coef_w)
    coef_ref[...] = jnp.concatenate(
        [
            jnp.concatenate([a_hi, a_hi, w_hi, w_hi, w_hi], axis=1),
            jnp.concatenate([a_mid, a_mid, w_mid, w_mid, jnp.zeros_like(w_mid)], axis=1),
        ],
        axis=0,
    )

    def placed(x, first):
        wide = jnp.concatenate([x, jnp.zeros((np_, LANES - np_), F32)], axis=1)
        return pltpu.roll(wide, first, 1)

    sent(last)
    c1_ref[...] = (h1 + placed(lt1.T, nb))[:, 0:nc]
    c2_ref[...] = (h2b + placed(h2q, nb) + placed(low2, nc))[:, 0 : nc + np_]


def product(per, np_, z2, coef_ref, c1_ref, c2_ref, q1_ref, q2_ref, o1_ref, o2_ref):
    n2 = 2 * np_
    width = per * LANES
    at = pl.ds(pl.multiple_of(pl.program_id(0) * width, width), width)
    o = lax.dot_general(coef_ref[...], z2[:, at], NN, preferred_element_type=F32)
    out = o[0:n2] + o[n2:]
    for i in range(per):
        q1_ref[:, i, :] = out[0:np_, i * LANES : (i + 1) * LANES]
        q2_ref[:, i, :] = out[np_:, i * LANES : (i + 1) * LANES]
    o1_ref[...] = c1_ref[...]
    o2_ref[...] = c2_ref[...]


def local(nz, nx, ny, basis, panel, rate_codes):
    nb, rows, width = basis.shape
    np_ = panel.shape[0]
    sites = rows * width * nz * nx * ny * 2
    nc, nt, flat, nm = nb + np_, 2 * nb + 2 * np_, rows * width, nx * 2
    dims = (nz, nx, ny, rows, nb, np_, 1.0 / sites)
    vm = pltpu.VMEM
    tile = lambda *n: vm((*n, LANES), F32)
    dma = pltpu.SemaphoreType.DMA
    scratch = [
        tile(rows + 2, nc), tile(rows + 2, np_), vm((4, rows, LANES), jnp.int32), tile(5, rows + 16),
        vm((8, LANES), jnp.int32), vm((8, LANES), jnp.int32),
        tile(nc), tile(nc), tile(nc), tile(nc), tile(np_), tile(np_), tile(np_), tile(np_),
        tile(rows, nb), vm((4 * nb, 2 * nb), F32), vm((2 * nt, 4 * np_), F32),
        tile(nm, 16), tile(nm, 16), tile(ny, 16), tile(nz, 16), tile(nm, 16),
        dma((3,)), dma((14,)), dma((14,)), dma((2 * nm + ny + nz,)), dma((2 * nm + ny + nz,)),
    ]
    vmem = pl.BlockSpec(memory_space=pltpu.VMEM)
    nz2 = 4 * nb + 6 * np_
    held = pl.pallas_call(
        functools.partial(kernel, dims),
        out_shape=(
            jax.ShapeDtypeStruct((nz2, flat), BF16),
            jax.ShapeDtypeStruct((4 * np_, nz2), BF16),
            jax.ShapeDtypeStruct((np_, nc), F32),
            jax.ShapeDtypeStruct((np_, nc + np_), F32),
        ),
        in_specs=[pl.BlockSpec(memory_space=pltpu.HBM)] * 3,
        out_specs=(vmem,) * 4,
        scratch_shapes=scratch,
        compiler_params=pltpu.CompilerParams(collective_id=0, has_side_effects=True, vmem_limit_bytes=24 << 20),
        cost_estimate=pl.CostEstimate(flops=10**9, bytes_accessed=4 << 20, transcendentals=0),
    )(*[pltpu.with_memory_space_constraint(v, pltpu.HBM) for v in (basis, panel, rate_codes)])
    per = min(32, rows)
    block = pl.BlockSpec((np_, per, width), lambda k: (0, k, 0))
    whole = lambda *shape: pl.BlockSpec(shape, lambda k: (0, 0))
    q1, q2, c1, c2 = pl.pallas_call(
        functools.partial(product, per, np_),
        grid=(rows // per,),
        out_shape=(
            jax.ShapeDtypeStruct((np_, rows, width), F32),
            jax.ShapeDtypeStruct((np_, rows, width), F32),
            jax.ShapeDtypeStruct((np_, nc), F32),
            jax.ShapeDtypeStruct((np_, nc + np_), F32),
        ),
        in_specs=[vmem] * 4,
        out_specs=(block, block, whole(np_, nc), whole(np_, nc + np_)),
        compiler_params=pltpu.CompilerParams(vmem_limit_bytes=16 << 20),
        cost_estimate=pl.CostEstimate(flops=10**9, bytes_accessed=4 << 20, transcendentals=0),
    )(*held)
    return (q1, q2, c1.T, c2.T)


def solution(mesh):
    nx = 4
    nz = mesh.shape["gx"] // nx
    ny = mesh.shape["gy"] // 2
    placed = P(None, "gx", "gy")
    return jax.shard_map(
        functools.partial(local, nz, nx, ny),
        mesh=mesh,
        in_specs=(placed, placed, placed),
        out_specs=(placed, placed, P(), P()),
        check_vma=False,
    )
```
